256 devices in a mesh: mats: 64 (over z, x, core), tp: 4 (over y).
Axes of the slice: x: 4, y: 4, z: 8, core: 2. Of those that a mesh axis runs over, the one named last changes fastest.
Arguments:
- grad: bfloat16 [3072, 16384], P('tp', 'mats'), may hold values from -40 to 40
- momentum: float32 [3072, 16384], P('tp', 'mats'), may hold values from -6 to 6
Outputs:
- update: bfloat16 [3072, 16384], P('tp', 'mats')
- new_momentum: float32 [3072, 16384], P('tp', 'mats')
The draws below stay inside these ranges and needn't reach their ends.
All inputs are finite; a program needn't handle non-finite values.
Results may differ from the reference program's by a relative error of at most 0.01.
Values may be sent and summed in bfloat16 or wider, within the bound.
A program may use at most 64 MiB of HBM per device.

```python
import math
import jax
import jax.numpy as jnp
from jax import lax

R = 3072
C = 16384
ITERS = 2


def draw_grad(key, part):
    keys = jax.random.split(jax.random.fold_in(key, 11), 3)
    position = jnp.arange(R, dtype=jnp.float32).reshape(R, 1) / (R - 1.0)
    rising = jnp.exp(math.log(0.1) * (1.0 - position))
    rough_rows = jax.random.uniform(keys[0], (R, 1), jnp.float32, 0.5, 1.0)
    row_scale = rising * rough_rows
    col_scale = jnp.exp(jax.random.uniform(keys[1], (1, C), jnp.float32, 0.0, math.log(10.0)))
    base = jax.random.normal(keys[2], (R, C), jnp.float32)
    base = jnp.clip(base, -4.0, 4.0)
    return (base * row_scale * col_scale).astype(jnp.bfloat16)


def level_of(own_key, extent, shards, low, largest):
    loudness = 1.0
    for dim, shards_of in shards:
        heights = jax.random.uniform(jax.random.fold_in(jax.random.fold_in(own_key, 6), dim), (shards_of,), jnp.float32, low / len(shards), largest / len(shards))
        loudness = loudness * jnp.repeat(jnp.exp(heights), extent[dim] // shards_of).reshape((-1,) + (1,) * (len(extent) - 1 - dim))
    return loudness


def normal_values(key, extent, width, reach, cuts=(), held_as=jnp.bfloat16):
    entries = width * jax.random.normal(key, extent, jnp.float32)
    if cuts:
        entries = entries * level_of(key, extent, cuts, -0.22, 0.18)
    return jnp.clip(entries, -reach, reach).astype(held_as)


def setup_inputs(seed: int = 0) -> dict:
    key_of = jax.random.split(jax.random.key(seed), 3)
    grad = draw_grad(jax.random.fold_in(key_of[2], 71), 0)
    momentum = normal_values(key_of[1], (R, C), 1.0, 6.0, ((0, 4), (1, 64)), jnp.float32)
    return {"grad": grad, "momentum": momentum}


momentum_beta = 0.95
first_coef = 3.4445
second_coef = -4.775
third_coef = 2.0315
shape_gain = 0.2
epsilon = 1e-06

def reference(grad, momentum):
    new_momentum = momentum_beta * momentum + grad.astype(jnp.float32)
    iterate = (grad.astype(jnp.float32) + momentum_beta * new_momentum).astype(jnp.bfloat16)
    for step in range(ITERS):
        gram = lax.dot_general(iterate, iterate, (((1,), (1,)), ((), ())), preferred_element_type=jnp.float32).astype(jnp.bfloat16)
        first = jnp.dot(gram, iterate, preferred_element_type=jnp.float32).astype(jnp.bfloat16)
        second = jnp.dot(gram, first, preferred_element_type=jnp.float32).astype(jnp.bfloat16)
        if step == 0:
            bound = jnp.max(lax.optimization_barrier(jnp.sum(jnp.abs(gram.astype(jnp.float32)), axis=1))) + epsilon
            root = lax.rsqrt(bound)
            mixed = first_coef * iterate.astype(jnp.float32) * root + second_coef * first.astype(jnp.float32) * root ** 3 + third_coef * second.astype(jnp.float32) * root ** 5
        else:
            mixed = first_coef * iterate.astype(jnp.float32) + second_coef * first.astype(jnp.float32) + third_coef * second.astype(jnp.float32)
        iterate = mixed.astype(jnp.bfloat16)
    update = (shape_gain * math.sqrt(max(R, C)) * iterate.astype(jnp.float32)).astype(jnp.bfloat16)
    return (update, new_momentum)
```

```python
import math

import jax
import jax.numpy as jnp
from jax import lax
from jax.experimental import pallas as pl
from jax.experimental.pallas import tpu as pltpu
from jax.sharding import Mesh
from jax.sharding import PartitionSpec as P

R = 3072
C = 16384
AX = {"z": "mats_0", "x": "mats_1", "c": "mats_2", "y": "tp"}
SIZES = {"z": 8, "x": 4, "c": 2, "y": 4}

momentum_beta = 0.95
first_coef = 3.4445
second_coef = -4.775
third_coef = 2.0315
shape_gain = 0.2
epsilon = 1e-06

BF = jnp.bfloat16
F32 = jnp.float32
MESH = pl.DeviceIdType.MESH


def around(s, d, n):
    d = d % n
    return s if d == 0 else lax.rem(s + d, n)


class Comm:
    def __init__(self, send_sems, recv_sems):
        self.send_sems, self.recv_sems = send_sems, recv_sems
        self.next_send = self.next_recv = self.most_send = self.most_recv = 0
        self.open = []

    def recv_index(self):
        self.next_recv += 1
        self.most_recv = max(self.most_recv, self.next_recv)
        return self.next_recv - 1

    def start(self, src, dst, axis, to, index=None):
        if index is None:
            index = self.recv_index()
        copy = pltpu.make_async_remote_copy(
            src_ref=src,
            dst_ref=dst,
            send_sem=self.send_sems.at[self.next_send],
            recv_sem=self.recv_sems.at[index],
            device_id={AX[axis]: to},
            device_id_type=MESH,
        )
        self.next_send += 1
        self.most_send = max(self.most_send, self.next_send)
        copy.start()
        self.open.append(copy)
        return index

    def wait(self, dst, index, axis, peer):
        pltpu.make_async_remote_copy(
            src_ref=dst,
            dst_ref=dst,
            send_sem=self.send_sems.at[0],
            recv_sem=self.recv_sems.at[index],
            device_id={AX[axis]: peer},
            device_id_type=MESH,
        ).wait_recv()

    def drain(self):
        for copy in self.open:
            copy.wait_send()
        self.open = []
        self.next_send = 0


def tree(comm, me, n, a1, a2, slot, arrived):
    n1, n2 = n[a1], (n[a2] if a2 else 1)
    s1, s2 = me[a1], (me[a2] if a2 else 0)
    held = {}

    def ref(d1, d2, h):
        return slot(around(s1, d1, n1), around(s2, d2, n2), h)

    def send(level, d1, d2, hop, way):
        axis, size, s = (a1, n1, s1) if level == 1 else (a2, n2, s2)
        half = None if hop < size // 2 else (0 if way > 0 else 1)
        piece = ref(d1, d2, half)
        index = comm.start(piece, piece, axis, around(s, way, size))
        key = (1, d1 - way, d2, hop, way) if level == 1 else (2, d1, d2 - way, hop, way)
        held[key] = (index, half)

    def take(level, d1, d2, hop, way):
        index, half = held.pop((level, d1, d2, hop, way))
        axis, size, s = (a1, n1, s1) if level == 1 else (a2, n2, s2)
        comm.wait(ref(d1, d2, half), index, axis, around(s, way, size))

    def spread(d1):
        if n2 > 1:
            for way in (1, -1):
                send(2, d1, 0, 1, way)

    if n1 > 1:
        for way in (1, -1):
            send(1, 0, 0, 1, way)
    spread(0)
    arrived(0, 0)
    yield
    last1, last2 = n1 // 2, n2 // 2
    for hop in range(1, last1 + last2 + 1):
        if n1 > 1 and hop <= last1:
            for way in (1, -1):
                d1 = -hop * way
                take(1, d1, 0, hop, way)
                if hop < last1:
                    send(1, d1, 0, hop + 1, way)
                    spread(d1)
                    arrived(d1, 0)
            if hop == last1:
                spread(last1)
                arrived(last1, 0)
        for t1 in range(last1 + 1):
            t2 = hop - t1
            if n2 == 1 or not 1 <= t2 <= last2:
                continue
            for d1 in [0] if t1 == 0 else [last1] if t1 == last1 else [-t1, t1]:
                for way in (1, -1):
                    d2 = -t2 * way
                    take(2, d1, d2, t2, way)
                    if t2 < last2:
                        send(2, d1, d2, t2 + 1, way)
                        arrived(d1, d2)
                if t2 == last2:
                    arrived(d1, last2)
        yield


def together(*walks):
    walks = list(walks)
    while walks:
        for walk in list(walks):
            try:
                next(walk)
            except StopIteration:
                walks.remove(walk)


def add_into(target, source):
    def step(i, carry):
        target[i] = (target[i].astype(F32) + source[i].astype(F32)).astype(BF)
        return carry

    if len(target.shape) > 2:
        lax.fori_loop(0, target.shape[0], step, 0)
    else:
        target[...] = (target[...].astype(F32) + source[...].astype(F32)).astype(BF)


def ring_sum(comm, me, n, axis, piece, landing):
    size, s = n[axis], me[axis]
    if size == 1:
        return
    last = size // 2
    index = {}
    for hop in range(1, last + 1):
        for way in (1, -1):
            first = 0 if way > 0 else 1
            d = around(s, way * (last - hop + 1), size)
            to, source = around(s, way, size), around(s, -way, size)
            half = first if hop == 1 else None
            if hop > 1:
                came = first if hop == 2 else None
                comm.wait(landing(way, hop - 1, came), index[way, hop - 1], axis, source)
                add_into(piece(d, came), landing(way, hop - 1, came))
            index[way, hop] = comm.start(piece(d, half), landing(way, hop, half), axis, to)
    for way in (1, -1):
        half = None if last > 1 else (0 if way > 0 else 1)
        comm.wait(landing(way, last, half), index[way, last], axis, around(s, -way, size))
    comm.drain()


def kernel(
    n, gain, x_ref, o_ref, xc, part, z1, x1, z2, x2, gram, cube, rpg, cpg, rp2, cp2, rpp, cpp, rph, cps, rpn, cpw,
    qi, swap, edge, peaks, send_sems, recv_sems, local_sem,
):
    nz, nx, nc, ny = n["z"], n["x"], n["c"], n["y"]
    me = {a: (lax.axis_index(AX[a]) if n[a] > 1 else 0) for a in "zxcy"}
    z, x, c, y = me["z"], me["x"], me["c"], me["y"]
    rows_block, columns = x_ref.shape
    rows_half = rows_block // nc
    ph, pw = gram.shape
    half_rows = ph // 2
    mine = (y * nc + c) * nx + x
    comm = Comm(send_sems, recv_sems)

    barrier = pltpu.get_barrier_semaphore()
    peers = [(a, d) for a in "zxcy" for d in range(1, n[a]) if a != "z" or d in (1, n[a] - 1)]
    for a, d in peers:
        pl.semaphore_signal(barrier, inc=1, device_id={AX[a]: around(me[a], d, n[a])}, device_id_type=MESH)
    pl.semaphore_wait(barrier, len(peers))

    parts = 2
    share = rows_block // parts

    def x_slot(i, q, h):
        if h is None:
            return xc.at[c, i, pl.ds(q * share, share)]
        return xc.at[c, i, pl.ds(q * share + h * (share // 2), share // 2)]

    own = pltpu.make_async_copy(x_ref, xc.at[c, y], local_sem)
    own.start()
    own.wait()
    to_partner = {}

    def x_arrived(q):
        def done(d, _):
            if nc > 1:
                ref = x_slot(around(y, d, ny), q, None)
                to_partner[q, d % ny] = comm.start(ref, ref, "c", 1 - c)

        return done

    together(*(tree(comm, me, n, "y", None, lambda i, _, h, q=q: x_slot(i, q, h), x_arrived(q)) for q in range(parts)))
    for (q, d), index in to_partner.items():
        comm.wait(xc.at[1 - c, around(y, d, ny), pl.ds(q * share, share)], index, "c", 1 - c)
    comm.drain()

    per_block = rows_block // pw

    def gram_piece(d, carry):
        total = jnp.zeros((rows_half, pw), F32)
        for h in range(nc):
            left = xc[h, y, pl.ds(pl.multiple_of(c * rows_half, rows_half), rows_half)]
            right = xc[h, d // per_block, pl.ds(pl.multiple_of(d % per_block * pw, pw), pw)]
            total += lax.dot_general(left, right, (((1,), (1,)), ((), ())), preferred_element_type=F32)
        part[d] = total.astype(BF).reshape(nx, ph, pw)
        return carry

    lax.fori_loop(0, nz, gram_piece, 0)

    def two_halves(ref, h, length):
        return ref if h is None else ref.at[pl.ds(h * length, length)]

    def finish(extra):
        total = part[z, x].astype(F32)
        for ref in extra:
            total += ref[...].astype(F32)
        gram[...] = total

    sums_base = comm.next_recv
    for core in range(nc):

        @pl.when(c == core)
        def _():
            comm.next_recv = sums_base
            if core == 0:
                ring_sum(
                    comm, me, n, "z",
                    lambda d, h: part.at[d] if h is None else part.at[d, pl.ds(h * (nx // 2), nx // 2)],
                    lambda way, hop, h: (
                        z1.at[int(way > 0), hop - 1] if h is None else z1.at[int(way > 0), hop - 1, pl.ds(h * (nx // 2), nx // 2)]
                    ),
                )
                if nz > 1:
                    for way in (0, 1):
                        add_into(part.at[z], z1.at[way, nz // 2 - 1])
                ring_sum(
                    comm, me, n, "x",
                    lambda d, h: two_halves(part.at[z, d], h, half_rows),
                    lambda way, hop, h: two_halves(x2.at[int(way > 0), hop - 1], h, half_rows),
                )
                finish([x2.at[way, nx // 2 - 1] for way in (0, 1)] if nx > 1 else [])
            else:
                ring_sum(
                    comm, me, n, "x",
                    lambda d, h: part.at[:, d] if h is None else part.at[pl.ds(h * (nz // 2), nz // 2), d],
                    lambda way, hop, h: (
                        x1.at[int(way > 0), hop - 1] if h is None else x1.at[int(way > 0), hop - 1, pl.ds(h * (nz // 2), nz // 2)]
                    ),
                )
                if nx > 1:
                    for way in (0, 1):
                        add_into(part.at[:, x], x1.at[way, nx // 2 - 1])
                ring_sum(
                    comm, me, n, "z",
                    lambda d, h: two_halves(part.at[d, x], h, half_rows),
                    lambda way, hop, h: two_halves(z2.at[int(way > 0), hop - 1], h, half_rows),
                )
                finish([z2.at[way, nz // 2 - 1] for way in (0, 1)] if nz > 1 else [])


    comm.next_recv = comm.most_recv

    def panels(rp, cp, base, peak=False):
        pieces = ny * nx
        for core in range(nc):

            @pl.when(c == core)
            def _():
                comm.next_recv = base + pieces + 1
                a1, a2 = ("y", "x") if core == 0 else ("x", "y")
                if n[a1] == 1:
                    a1, a2 = a2, a1

                def spot(i1, i2):
                    iy, ix = (i1, i2) if a1 == "y" else (i2, i1)
                    return (iy * nc + core) * nx + ix

                def slot(i1, i2, h):
                    return two_halves(cp.at[spot(i1, i2)], h, half_rows)

                def arrived(d1, d2):
                    if nc > 1:
                        dy, dx = (d1, d2) if a1 == "y" else (d2, d1)
                        ref = slot(around(me[a1], d1, n[a1]), around(me[a2], d2, n[a2]), None)
                        comm.start(ref, ref, "c", 1 - c, base + dy % ny * nx + dx % nx)

                def largest():
                    yield
                    kept = edge[0]
                    for axis, at in (("y", 1), ("x", 1 + ny), ("c", 1 + ny + nx)):
                        if n[axis] == 1:
                            continue
                        edge[at] = kept
                        index = {}
                        for d in range(1, n[axis]):
                            index[d] = comm.start(
                                edge.at[at], edge.at[at + d], axis, around(me[axis], d, n[axis]),
                                base + pieces if axis == "c" else None,
                            )
                        yield
                        for d in range(1, n[axis]):
                            comm.wait(edge.at[at + d], index[d], axis, around(me[axis], -d, n[axis]))
                            kept = jnp.maximum(kept, edge[at + d])
                    peaks[...] = kept

                walks = [
                    tree(comm, me, n, "z", None, lambda i, _, h: two_halves(rp.at[i], h, half_rows), lambda d, _: None),
                    tree(comm, me, n, a1, a2, slot, arrived),
                ]
                together(*walks, *([largest()] if peak else []))
                if nc > 1:
                    for dy in range(ny):
                        for dx in range(nx):
                            ref = cp.at[(around(y, dy, ny) * nc + 1 - core) * nx + around(x, dx, nx)]
                            comm.wait(ref, base + dy * nx + dx, "c", 1 - c)
                comm.drain()

        comm.next_recv = max(comm.next_recv, comm.most_recv)

    def put(value, rp, cp):
        value = value.astype(BF)
        if rp is not None:
            rp[z] = value
        if cp is not None:
            cp[mine] = value

    per_chunk = cpg.shape[0] // nz

    def times(rps, cp):
        def step(k, totals):
            right = cp[pl.ds(k * per_chunk, per_chunk)].reshape(per_chunk * ph, pw)
            return tuple(t + jnp.dot(rp[k], right, preferred_element_type=F32) for t, rp in zip(totals, rps))

        return lax.fori_loop(0, nz, step, tuple(jnp.zeros((ph, pw), F32) for _ in rps))

    def with_identity(value, row, column, scale):
        rows = lax.broadcasted_iota(jnp.int32, value.shape, 0) + row
        across = lax.broadcasted_iota(jnp.int32, value.shape, 1) + column
        return value + jnp.where(rows == across, scale, 0.0)

    put(gram[...], rpg, cpg)
    panels(rpg, cpg, comm.next_recv)

    def sizes(k, total):
        return total + jnp.abs(rpg[k].astype(F32))

    row_sums = jnp.sum(lax.fori_loop(0, nz, sizes, jnp.zeros((ph, pw), F32)), axis=1, keepdims=True)
    edge[0] = jnp.broadcast_to(jnp.max(row_sums, axis=0, keepdims=True), edge.shape[1:])
    (square,) = times([rpg], cpg)
    put(square, rp2, cp2)
    panels(rp2, cp2, comm.next_recv, peak=True)

    bound = jnp.max(jnp.max(peaks[...], axis=1, keepdims=True), axis=0, keepdims=True) + epsilon
    inverse = 1.0 / bound
    root = lax.rsqrt(bound)

    def mix(once, twice, row, column):
        value = second_coef * (once.astype(F32) * inverse) + third_coef * (twice.astype(F32) * inverse * inverse)
        return with_identity(value, row, column, first_coef)

    def mix_rows(k, carry):
        rpp[k] = mix(rpg[k], rp2[k], mine * ph, k * pw).astype(BF)
        return carry

    def mix_columns(k, carry):
        cpp[k] = mix(cpg[k], cp2[k], k * ph, z * pw).astype(BF)
        return carry

    lax.fori_loop(0, nz, mix_rows, 0)
    lax.fori_loop(0, cpp.shape[0], mix_columns, 0)
    cube[...] = mix(gram[...], square, mine * ph, z * pw)

    (once,) = times([rpg], cpp)
    (twice,) = times([rpp], cpp)
    put(once * inverse, rph, None)
    put(twice, None, cps)
    panels(rph, cps, comm.next_recv)
    (next_gram,) = times([rph], cpp)
    (next_first,) = times([rph], cps)
    put(next_gram, rpn, None)
    put(next_first, None, cpw)
    panels(rpn, cpw, comm.next_recv)
    (next_second,) = times([rpn], cpw)
    whole = (gain * root) * (first_coef * cube[...] + second_coef * next_first + third_coef * next_second)
    qi[z, x] = whole.astype(BF)

    sums_base = comm.next_recv
    for core in range(nc):

        @pl.when(c == core)
        def _():
            comm.next_recv = sums_base
            a1, a2 = ("z", "x") if core == 0 else ("x", "z")
            if n[a1] == 1:
                a1, a2 = a2, a1

            def slot(i1, i2, h):
                iz, ix = (i1, i2) if a1 == "z" else (i2, i1)
                return two_halves(qi.at[iz, ix], h, half_rows)

            together(tree(comm, me, n, a1, a2, slot, lambda d1, d2: None))
            comm.drain()

    comm.next_recv = comm.most_recv

    def product(side):
        def step(k, total):
            left = qi[k].reshape(rows_half, pw)
            right = xc[side, k // per_block, pl.ds(pl.multiple_of(k % per_block * pw, pw), pw)]
            return total + jnp.dot(left, right, preferred_element_type=F32)

        return lax.fori_loop(0, nz, step, jnp.zeros((rows_half, columns), F32)).astype(BF)

    if nc > 1:
        swap[0] = product(1 - c)
        index = comm.start(swap.at[0], swap.at[1], "c", 1 - c)
    o_ref[pl.ds(pl.multiple_of(c * rows_half, rows_half), rows_half)] = product(c)
    if nc > 1:
        comm.wait(swap.at[1], index, "c", 1 - c)
        o_ref[pl.ds(pl.multiple_of((1 - c) * rows_half, rows_half), rows_half)] = swap[1]
        comm.drain()


def update_call(n, gain, x):
    nz, nx, nc, ny = n["z"], n["x"], n["c"], n["y"]
    rows_block, columns = x.shape
    rows = rows_block * ny
    ph, pw = rows // (ny * nc * nx), rows // nz
    pieces = ny * nc * nx
    row_panel = pltpu.VMEM((nz, ph, pw), BF)
    column_panel = pltpu.VMEM((pieces, ph, pw), BF)
    hops_z, hops_x = max(nz // 2, 1), max(nx // 2, 1)
    tiles = 2 + ny + nx + nc
    return pl.pallas_call(
        lambda *refs: kernel(n, gain, *refs),
        out_shape=jax.ShapeDtypeStruct(x.shape, BF),
        in_specs=[pl.BlockSpec(memory_space=pltpu.VMEM)],
        out_specs=pl.BlockSpec(memory_space=pltpu.VMEM),
        scratch_shapes=[
            pltpu.VMEM((nc, ny, rows_block, columns), BF),
            pltpu.VMEM((nz, nx, ph, pw), BF),
            pltpu.VMEM((2, hops_z, nx, ph, pw), BF),
            pltpu.VMEM((2, hops_x, nz, ph, pw), BF),
            pltpu.VMEM((2, hops_z, ph, pw), BF),
            pltpu.VMEM((2, hops_x, ph, pw), BF),
            pltpu.VMEM((ph, pw), F32),
            pltpu.VMEM((ph, pw), F32),
            row_panel, column_panel, row_panel, column_panel, row_panel, column_panel,
            row_panel, column_panel, row_panel, column_panel,
            pltpu.VMEM((nz, nx, ph, pw), BF),
            pltpu.VMEM((2, rows_block // nc, columns), BF),
            pltpu.VMEM((tiles, 8, 128), F32),
            pltpu.VMEM((8, 128), F32),
            pltpu.SemaphoreType.DMA((80,)),
            pltpu.SemaphoreType.DMA((300,)),
            pltpu.SemaphoreType.DMA,
        ],
        compiler_params=pltpu.CompilerParams(
            collective_id=0, has_side_effects=True, vmem_limit_bytes=48 * 1024 * 1024
        ),
    )(x)


def per_device(grad, momentum):
    new_momentum = momentum_beta * momentum + grad.astype(F32)
    iterate = (grad.astype(F32) + momentum_beta * new_momentum).astype(BF)
    update = update_call(SIZES, shape_gain * math.sqrt(max(R, C)), iterate)
    return (update, new_momentum)


def solution(mesh):
    devices = mesh.devices.reshape(SIZES["z"], SIZES["x"], SIZES["c"], SIZES["y"])
    split = Mesh(devices, (AX["z"], AX["x"], AX["c"], AX["y"]))
    mats = (AX["z"], AX["x"], AX["c"])
    return jax.shard_map(
        per_device,
        mesh=split,
        in_specs=(P(AX["y"], mats), P(AX["y"], mats)),
        out_specs=(P(AX["y"], mats), P(AX["y"], mats)),
        check_vma=False,
    )
```

```python
import math

import jax
import jax.numpy as jnp
from jax import lax
from jax.experimental import pallas as pl
from jax.experimental.pallas import tpu as pltpu
from jax.sharding import Mesh
from jax.sharding import PartitionSpec as P

R = 3072
C = 16384
AX = {"z": "mats_0", "x": "mats_1", "c": "mats_2", "y": "tp"}
SIZES = {"z": 8, "x": 4, "c": 2, "y": 4}

momentum_beta = 0.95
first_coef = 3.4445
second_coef = -4.775
third_coef = 2.0315
shape_gain = 0.2
epsilon = 1e-06

BF = jnp.bfloat16
F32 = jnp.float32
MESH = pl.DeviceIdType.MESH


def around(s, d, n):
    d = d % n
    return s if d == 0 else lax.rem(s + d, n)


class Comm:
    def __init__(self, send_sems, recv_sems):
        self.send_sems, self.recv_sems = send_sems, recv_sems
        self.next_send = self.next_recv = self.most_recv = 0
        self.open = []

    def recv_index(self):
        self.next_recv += 1
        self.most_recv = max(self.most_recv, self.next_recv)
        return self.next_recv - 1

    def send_index(self):
        self.next_send += 1
        return self.next_send - 1

    def start(self, src, dst, axis, to, index=None, send=None):
        if index is None:
            index = self.recv_index()
        kept = send is None
        if kept:
            send = self.send_index()
        copy = pltpu.make_async_remote_copy(
            src_ref=src,
            dst_ref=dst,
            send_sem=self.send_sems.at[send],
            recv_sem=self.recv_sems.at[index],
            device_id={AX[axis]: to},
            device_id_type=MESH,
        )
        copy.start()
        if kept:
            self.open.append(copy)
        return index

    def handle(self, ref, send, index, axis, peer):
        return pltpu.make_async_remote_copy(
            src_ref=ref,
            dst_ref=ref,
            send_sem=self.send_sems.at[send],
            recv_sem=self.recv_sems.at[index],
            device_id={AX[axis]: peer},
            device_id_type=MESH,
        )

    def wait(self, ref, index, axis, peer):
        self.handle(ref, 0, index, axis, peer).wait_recv()

    def wait_sent(self, ref, send, axis, peer):
        self.handle(ref, send, 0, axis, peer).wait_send()

    def drain(self):
        for copy in self.open:
            copy.wait_send()
        self.next_send -= len(self.open)
        self.open = []


def ring_relay(comm, me, n, axis, slot, arrived):
    size, s = n[axis], me[axis]
    at = lambda d: around(s, d, size)
    send = comm.send_index()
    near, far = comm.recv_index(), {1: comm.recv_index(), -1: comm.recv_index()}
    own = slot(s, None)
    for way in (1, -1):
        comm.start(own, own, axis, at(2 * way), far[way], send)
    for way in (1, -1):
        comm.start(own, own, axis, at(way), near, send)
    yield
    for way in (1, -1):
        piece = slot(at(-2 * way), None)
        comm.wait(piece, far[way], axis, at(-2 * way))
        comm.start(piece, piece, axis, at(way), near, send)
        half = slot(at(-2 * way), 0 if way > 0 else 1)
        comm.start(half, half, axis, at(2 * way), near, send)
    yield
    arrived(near, send)


def tree(comm, me, n, a1, a2, slot, arrived):
    n1, n2 = n[a1], (n[a2] if a2 else 1)
    s1, s2 = me[a1], (me[a2] if a2 else 0)
    held = {}

    def ref(d1, d2, h):
        return slot(around(s1, d1, n1), around(s2, d2, n2), h)

    def send(level, d1, d2, hop, way):
        axis, size, s = (a1, n1, s1) if level == 1 else (a2, n2, s2)
        half = None if hop < size // 2 else (0 if way > 0 else 1)
        piece = ref(d1, d2, half)
        index = comm.start(piece, piece, axis, around(s, way, size))
        key = (1, d1 - way, d2, hop, way) if level == 1 else (2, d1, d2 - way, hop, way)
        held[key] = (index, half)

    def take(level, d1, d2, hop, way):
        index, half = held.pop((level, d1, d2, hop, way))
        axis, size, s = (a1, n1, s1) if level == 1 else (a2, n2, s2)
        comm.wait(ref(d1, d2, half), index, axis, around(s, way, size))

    def spread(d1):
        if n2 > 1:
            for way in (1, -1):
                send(2, d1, 0, 1, way)

    if n1 > 1:
        for way in (1, -1):
            send(1, 0, 0, 1, way)
    spread(0)
    arrived(0, 0)
    yield
    last1, last2 = n1 // 2, n2 // 2
    for hop in range(1, last1 + last2 + 1):
        if n1 > 1 and hop <= last1:
            for way in (1, -1):
                d1 = -hop * way
                take(1, d1, 0, hop, way)
                if hop < last1:
                    send(1, d1, 0, hop + 1, way)
                    spread(d1)
                    arrived(d1, 0)
            if hop == last1:
                spread(last1)
                arrived(last1, 0)
        for t1 in range(last1 + 1):
            t2 = hop - t1
            if n2 == 1 or not 1 <= t2 <= last2:
                continue
            for d1 in [0] if t1 == 0 else [last1] if t1 == last1 else [-t1, t1]:
                for way in (1, -1):
                    d2 = -t2 * way
                    take(2, d1, d2, t2, way)
                    if t2 < last2:
                        send(2, d1, d2, t2 + 1, way)
                        arrived(d1, d2)
                if t2 == last2:
                    arrived(d1, last2)
        yield


def together(*walks):
    walks = list(walks)
    while walks:
        for walk in list(walks):
            try:
                next(walk)
            except StopIteration:
                walks.remove(walk)


def kernel(
    n, gain, x_ref, o_ref, xc, part, z1, x1, z2, x2, gram, cube, sums, rpg, cpg, rp2, cp2, rpp, cpp, rph, cps, rpn, cpw,
    qi, swap, edge, peaks, send_sems, recv_sems, local_sem,
):
    nz, nx, nc, ny = n["z"], n["x"], n["c"], n["y"]
    me = {a: (lax.axis_index(AX[a]) if n[a] > 1 else 0) for a in "zxcy"}
    z, x, c, y = me["z"], me["x"], me["c"], me["y"]
    rows_block, columns = x_ref.shape
    rows_half = rows_block // nc
    ph, pw = gram.shape
    half_rows = ph // 2
    mine = (y * nc + c) * nx + x
    comm = Comm(send_sems, recv_sems)

    barrier = pltpu.get_barrier_semaphore()
    peers = [(a, d) for a in "zxcy" for d in range(1, n[a])]
    for a, d in peers:
        pl.semaphore_signal(barrier, inc=1, device_id={AX[a]: around(me[a], d, n[a])}, device_id_type=MESH)
    pl.semaphore_wait(barrier, len(peers))

    parts = 2
    share = rows_block // parts

    def x_slot(i, q, h):
        if h is None:
            return xc.at[c, i, pl.ds(q * share, share)]
        return xc.at[c, i, pl.ds(q * share + h * (share // 2), share // 2)]

    own = pltpu.make_async_copy(x_ref, xc.at[c, y], local_sem)
    own.start()
    own.wait()
    to_partner = {}

    def x_arrived(q):
        def done(d, _):
            if nc > 1:
                ref = x_slot(around(y, d, ny), q, None)
                to_partner[q, d % ny] = comm.start(ref, ref, "c", 1 - c)

        return done

    together(*(tree(comm, me, n, "y", None, lambda i, _, h, q=q: x_slot(i, q, h), x_arrived(q)) for q in range(parts)))
    for (q, d), index in to_partner.items():
        comm.wait(xc.at[1 - c, around(y, d, ny), pl.ds(q * share, share)], index, "c", 1 - c)
    comm.drain()

    per_block = rows_block // pw
    top = pl.multiple_of(c * rows_half, rows_half)

    def right_rows(h, d):
        return xc[h, d // per_block, pl.ds(pl.multiple_of(d % per_block * pw, pw), pw)]

    def outer(left, right):
        return lax.dot_general(left, right, (((1,), (1,)), ((), ())), preferred_element_type=F32)

    def part_columns(d):
        total = sum(outer(xc[h, y, pl.ds(top, rows_half)], right_rows(h, d)) for h in range(nc))
        part[d] = total.astype(BF).reshape(nx, ph, pw)

    def part_rows(d):
        rows = pl.ds(pl.multiple_of(top + d * ph, ph), ph)

        def step(k, carry):
            part[k, d] = sum(outer(xc[h, y, rows], right_rows(h, k)) for h in range(nc)).astype(BF)
            return carry

        lax.fori_loop(0, nz, step, 0)

    def plus(piece, *more):
        total = piece[...].astype(F32)
        for other in more:
            total += other[...].astype(F32)
        return total

    def plane_sum(axis, piece, landing, chunks, prepare, across, final_landing):
        size, s = n[axis], me[axis]
        last = size // 2
        halves = {1: chunks[: len(chunks) // 2], -1: chunks[len(chunks) // 2 :]}
        index = {}
        send, final_send, final = comm.send_index(), comm.send_index(), comm.recv_index()

        def go(way, hop, e):
            index[way, hop, e] = comm.recv_index()
            d = around(s, way * (last - hop + 1), size)
            comm.start(piece(d, e), landing(way, hop, e), axis, around(s, way, size), index[way, hop, e], send)

        def come(way, hop, e):
            comm.wait(landing(way, hop, e), index[way, hop, e], axis, around(s, -way, size))
            return landing(way, hop, e)

        prepare(around(s, last, size))
        for a, b in zip(halves[1], halves[-1]):
            go(1, 1, a)
            go(-1, 1, b)
        for hop in range(2, last + 1):
            for way in (1, -1):
                prepare(around(s, way * (last - hop + 1), size))
                if hop == 2:
                    for e in halves[-way]:
                        go(way, hop, e)
            for k in range(len(chunks)):
                for way in (1, -1):
                    order = halves[way] if hop == 2 else halves[-way] + halves[way]
                    if k < len(order):
                        e = order[k]
                        ref = piece(around(s, way * (last - hop + 1), size), e)
                        ref[...] = plus(ref, come(way, hop - 1, e)).astype(BF)
                        go(way, hop, e)
        prepare(s)
        order = [e for pair in zip(halves[1], halves[-1]) for e in pair]
        for e in order:
            ref = piece(s, e)
            total = plus(ref, come(1, last, e), come(-1, last, e))
            if e == 0:
                gram[...] = total
            else:
                ref[...] = total.astype(BF)
                comm.start(ref, final_landing.at[e - 1], across, around(me[across], e, n[across]), final, final_send)
        comm.wait(final_landing, final, across, around(me[across], 1, n[across]))
        gram[...] = plus(gram, *(final_landing.at[k] for k in range(n[across] - 1)))
        comm.wait_sent(blocks((size - 1) * len(chunks)), send, axis, around(s, 1, size))
        comm.wait_sent(final_landing, final_send, across, around(me[across], 1, n[across]))

    def two_halves(ref, h, length):
        return ref if h is None else ref.at[pl.ds(h * length, length)]

    def blocks(count):
        across = next(k for k in range(nx, 0, -1) if count % k == 0 and count // k <= nz)
        return part.at[pl.ds(0, count // across), pl.ds(0, across)]

    base_recv, base_send = comm.next_recv, comm.next_send
    for core in range(nc):

        @pl.when(c == core)
        def _():
            comm.next_recv, comm.next_send = base_recv, base_send
            if core == 0:
                plane_sum(
                    "z", lambda d, e: part.at[d, around(x, e, nx)], lambda way, hop, e: z1.at[int(way > 0), hop - 1, e],
                    [2, 1, 3, 0], part_columns, "x", x2,
                )
            else:
                plane_sum(
                    "x", lambda d, e: part.at[around(z, e, nz), d], lambda way, hop, e: x1.at[int(way > 0), hop - 1, e],
                    [4, 5, 2, 7, 3, 6, 1, 0], part_rows, "z", z2,
                )

    comm.next_recv = comm.most_recv

    unsent = []

    def panels(rp, cp, half_done, peak=False):
        base_recv, base_send = comm.next_recv, comm.next_send
        for core in range(nc):

            @pl.when(c == core)
            def _():
                comm.next_recv, comm.next_send = base_recv, base_send
                over, peak_over = comm.recv_index(), comm.recv_index()
                send, send_over = comm.send_index(), comm.send_index()
                a1, a2 = ("y", "x") if core == 0 else ("x", "y")
                n1, n2 = n[a1], n[a2]
                at1, at2 = (lambda d: around(me[a1], d, n1)), (lambda d: around(me[a2], d, n2))

                def spot(d1, d2, h=None):
                    iy, ix = (at1(d1), at2(d2)) if a1 == "y" else (at2(d2), at1(d1))
                    return cp.at[iy, core, ix] if h is None else cp.at[iy, core, ix, pl.ds(h * half_rows, half_rows)]

                def group(d2):
                    return cp.at[:, core, at2(d2)] if a1 == "y" else cp.at[at2(d2), core]

                def to_partner(d2):
                    comm.start(group(d2), group(d2), "c", 1 - c, over, send_over)

                near1, far1, last = comm.recv_index(), comm.recv_index(), comm.recv_index()
                hop2 = {(way, k): comm.recv_index() for way in (1, -1) for k in range(3)}

                def spread(d1, k):
                    for way in (1, -1):
                        comm.start(spot(d1, 0), spot(d1, 0), a2, at2(way), hop2[way, k], send)
                    if d1 == 2:
                        comm.start(spot(d1, 0), spot(d1, 0), a2, at2(2), last, send)

                def pass_on(way, d1s):
                    for d1 in d1s:
                        half = spot(d1, -way, 0 if way > 0 else 1)
                        comm.start(half, half, a2, at2(way), last, send)

                def several(count):
                    return blocks(count)

                z_left = []
                z_walk = ring_relay(
                    comm, me, n, "z", lambda i, h: two_halves(rp.at[i], h, half_rows), lambda *left: z_left.append(left)
                )
                own = spot(0, 0)
                comm.start(own, own, a1, at1(2), far1, send)
                for way in (1, -1):
                    comm.start(own, own, a1, at1(way), near1, send)
                next(z_walk)
                spread(0, 0)
                peak_walk = largest(peak_over) if peak else iter(())
                next(peak_walk, None)

                comm.wait(several(2), near1, a1, at1(1))
                spread(-1, 1)
                spread(1, 1)
                for way in (1, -1):
                    comm.wait(own, hop2[way, 0], a2, at2(way))
                    pass_on(way, [0])
                comm.wait(own, far1, a1, at1(2))
                spread(2, 2)
                to_partner(0)
                next(z_walk)
                next(peak_walk, None)
                for way in (1, -1):
                    comm.wait(several(2), hop2[way, 1], a2, at2(way))
                    pass_on(way, [-1, 1])
                for way in (1, -1):
                    comm.wait(own, hop2[way, 2], a2, at2(way))
                    to_partner(-way)
                next(peak_walk, None)
                next(z_walk, None)
                comm.wait(several(4), last, a2, at2(1))
                to_partner(2)
                ((near, z_send),) = z_left
                comm.wait(rp.at[pl.ds(0, nz - 3)], near, "z", around(z, 1, nz))
                next(peak_walk, None)
                half_done()
                comm.wait(several(16), over, "c", 1 - c)
                if core == 0:
                    unsent.append((7, z_send, "z"))
                    unsent.append((15, send, "y"))
                    unsent.append((16, send_over, "c"))

        comm.next_recv = comm.most_recv

    def largest(over):
        kept = edge[0]
        sends = []
        for axis, at in (("y", 1), ("x", 1 + ny), ("c", 1 + ny + nx)):
            edge[at] = kept
            index, send = over if axis == "c" else comm.recv_index(), comm.send_index()
            for d in range(1, n[axis]):
                comm.start(edge.at[at], edge.at[at + d], axis, around(me[axis], d, n[axis]), index, send)
            yield
            comm.wait(edge.at[pl.ds(at + 1, n[axis] - 1)], index, axis, around(me[axis], 1, n[axis]))
            comm.wait_sent(edge.at[pl.ds(at + 1, n[axis] - 1)], send, axis, around(me[axis], 1, n[axis]))
            for d in range(1, n[axis]):
                kept = jnp.maximum(kept, edge[at + d])
        peaks[...] = kept

    def put(value, rp, cp):
        value = value.astype(BF)
        if rp is not None:
            rp[z] = value
        if cp is not None:
            cp[y, c, x] = value

    def times(rps, cp, core=None, totals=None):
        def step(k, totals):
            at = k if core is None else k * nc + core
            right = cp[at // nc, at % nc].reshape(nx * ph, pw)
            return tuple(t + jnp.dot(rp[at], right, preferred_element_type=F32) for t, rp in zip(totals, rps))

        if totals is None:
            totals = tuple(jnp.zeros((ph, pw), F32) for _ in rps)
        return lax.fori_loop(0, nz if core is None else nz // nc, step, totals)

    def exchange_and_times(rp, cp, pairs, peak=False):
        def half_done():
            at = 0
            for rps, right in pairs:
                for total in times(rps, right, c):
                    sums[at] = total
                    at += 1

        panels(rp, cp, half_done, peak)
        results, at = [], 0
        for rps, right in pairs:
            results += times(rps, right, 1 - c, tuple(sums[at + k] for k in range(len(rps))))
            at += len(rps)
        return results

    def with_identity(value, row, column, scale):
        rows = lax.broadcasted_iota(jnp.int32, value.shape, 0) + row
        across = lax.broadcasted_iota(jnp.int32, value.shape, 1) + column
        return value + jnp.where(rows == across, scale, 0.0)

    put(gram[...], rpg, cpg)
    (square,) = exchange_and_times(rpg, cpg, [([rpg], cpg)])

    def sizes(k, total):
        return total + jnp.abs(rpg[k].astype(F32))

    row_sums = jnp.sum(lax.fori_loop(0, nz, sizes, jnp.zeros((ph, pw), F32)), axis=1, keepdims=True)
    edge[0] = jnp.broadcast_to(jnp.max(row_sums, axis=0, keepdims=True), edge.shape[1:])
    put(square, rp2, cp2)
    panels(rp2, cp2, lambda: None, peak=True)

    bound = jnp.max(jnp.max(peaks[...], axis=1, keepdims=True), axis=0, keepdims=True) + epsilon
    inverse = 1.0 / bound
    root = lax.rsqrt(bound)

    def mix(once, twice, row, column):
        value = second_coef * (once.astype(F32) * inverse) + third_coef * (twice.astype(F32) * inverse * inverse)
        return with_identity(value, row, column, first_coef)

    def mix_rows(k, carry):
        rpp[k] = mix(rpg[k], rp2[k], mine * ph, k * pw).astype(BF)
        return carry

    def mix_columns(k, carry):
        at = (k // (nc * nx), k // nx % nc, k % nx)
        cpp[at] = mix(cpg[at], cp2[at], k * ph, z * pw).astype(BF)
        return carry

    lax.fori_loop(0, nz, mix_rows, 0)
    lax.fori_loop(0, ny * nc * nx, mix_columns, 0)
    cube[...] = mix(gram[...], square, mine * ph, z * pw)

    once, twice = times([rpg, rpp], cpp)
    put(once * inverse, rph, None)
    put(twice, None, cps)
    next_gram, next_first = exchange_and_times(rph, cps, [([rph], cpp), ([rph], cps)])
    put(next_gram, rpn, None)
    put(next_first, None, cpw)
    (next_second,) = exchange_and_times(rpn, cpw, [([rpn], cpw)])
    whole = (gain * root) * (first_coef * cube[...] + second_coef * next_first + third_coef * next_second)
    qi[z, x] = whole.astype(BF)

    sums_base = comm.next_recv
    for core in range(nc):

        @pl.when(c == core)
        def _():
            comm.next_recv = sums_base
            a1, a2 = ("z", "x") if core == 0 else ("x", "z")
            if n[a1] == 1:
                a1, a2 = a2, a1

            def slot(i1, i2, h):
                iz, ix = (i1, i2) if a1 == "z" else (i2, i1)
                return two_halves(qi.at[iz, ix], h, half_rows)

            together(tree(comm, me, n, a1, a2, slot, lambda d1, d2: None))
            comm.drain()

    comm.next_recv = comm.most_recv

    def product(side):
        def step(k, total):
            left = qi[k].reshape(rows_half, pw)
            right = xc[side, k // per_block, pl.ds(pl.multiple_of(k % per_block * pw, pw), pw)]
            return total + jnp.dot(left, right, preferred_element_type=F32)

        return lax.fori_loop(0, nz, step, jnp.zeros((rows_half, columns), F32)).astype(BF)

    if nc > 1:
        swap[0] = product(1 - c)
        index = comm.start(swap.at[0], swap.at[1], "c", 1 - c)
    o_ref[pl.ds(pl.multiple_of(c * rows_half, rows_half), rows_half)] = product(c)
    if nc > 1:
        comm.wait(swap.at[1], index, "c", 1 - c)
        o_ref[pl.ds(pl.multiple_of((1 - c) * rows_half, rows_half), rows_half)] = swap[1]
        comm.drain()
    for count, send, axis in unsent:
        comm.wait_sent(rpg.at[pl.ds(0, count)] if count < nz else blocks(count), send, axis, around(me[axis], 1, n[axis]))


def update_call(n, gain, x):
    nz, nx, nc, ny = n["z"], n["x"], n["c"], n["y"]
    rows_block, columns = x.shape
    rows = rows_block * ny
    ph, pw = rows // (ny * nc * nx), rows // nz
    row_panel = pltpu.VMEM((nz, ph, pw), BF)
    column_panel = pltpu.VMEM((ny, nc, nx, ph, pw), BF)
    hops_z, hops_x = max(nz // 2, 1), max(nx // 2, 1)
    tiles = 2 + ny + nx + nc
    return pl.pallas_call(
        lambda *refs: kernel(n, gain, *refs),
        out_shape=jax.ShapeDtypeStruct(x.shape, BF),
        in_specs=[pl.BlockSpec(memory_space=pltpu.VMEM)],
        out_specs=pl.BlockSpec(memory_space=pltpu.VMEM),
        scratch_shapes=[
            pltpu.VMEM((nc, ny, rows_block, columns), BF),
            pltpu.VMEM((nz, nx, ph, pw), BF),
            pltpu.VMEM((2, hops_z, nx, ph, pw), BF),
            pltpu.VMEM((2, hops_x, nz, ph, pw), BF),
            pltpu.VMEM((nz - 1, ph, pw), BF),
            pltpu.VMEM((nx - 1, ph, pw), BF),
            pltpu.VMEM((ph, pw), F32),
            pltpu.VMEM((ph, pw), F32),
            pltpu.VMEM((2, ph, pw), F32),
            row_panel, column_panel, row_panel, column_panel, row_panel, column_panel,
            row_panel, column_panel, row_panel, column_panel,
            pltpu.VMEM((nz, nx, ph, pw), BF),
            pltpu.VMEM((2, rows_block // nc, columns), BF),
            pltpu.VMEM((tiles, 8, 128), F32),
            pltpu.VMEM((8, 128), F32),
            pltpu.SemaphoreType.DMA((80,)),
            pltpu.SemaphoreType.DMA((300,)),
            pltpu.SemaphoreType.DMA,
        ],
        compiler_params=pltpu.CompilerParams(
            collective_id=0, has_side_effects=True, vmem_limit_bytes=48 * 1024 * 1024
        ),
    )(x)


def per_device(grad, momentum):
    new_momentum = momentum_beta * momentum + grad.astype(F32)
    iterate = (grad.astype(F32) + momentum_beta * new_momentum).astype(BF)
    update = update_call(SIZES, shape_gain * math.sqrt(max(R, C)), iterate)
    return (update, new_momentum)


def solution(mesh):
    devices = mesh.devices.reshape(SIZES["z"], SIZES["x"], SIZES["c"], SIZES["y"])
    split = Mesh(devices, (AX["z"], AX["x"], AX["c"], AX["y"]))
    mats = (AX["z"], AX["x"], AX["c"])
    return jax.shard_map(
        per_device,
        mesh=split,
        in_specs=(P(AX["y"], mats), P(AX["y"], mats)),
        out_specs=(P(AX["y"], mats), P(AX["y"], mats)),
        check_vma=False,
    )
```

```python
import math

import jax
import jax.numpy as jnp
from jax import lax
from jax.experimental import pallas as pl
from jax.experimental.pallas import tpu as pltpu
from jax.sharding import Mesh
from jax.sharding import PartitionSpec as P

R = 3072
C = 16384
AX = {"z": "mats_0", "x": "mats_1", "c": "mats_2", "y": "tp"}
SIZES = {"z": 8, "x": 4, "c": 2, "y": 4}

momentum_beta = 0.95
first_coef = 3.4445
second_coef = -4.775
third_coef = 2.0315
shape_gain = 0.2
epsilon = 1e-06

BF = jnp.bfloat16
F32 = jnp.float32
MESH = pl.DeviceIdType.MESH


def around(s, d, n):
    d = d % n
    return s if d == 0 else lax.rem(s + d, n)


class Comm:
    def __init__(self, send_sems, recv_sems):
        self.send_sems, self.recv_sems = send_sems, recv_sems
        self.next_send = self.next_recv = self.most_recv = 0
        self.open = []

    def recv_index(self):
        self.next_recv += 1
        self.most_recv = max(self.most_recv, self.next_recv)
        return self.next_recv - 1

    def send_index(self):
        self.next_send += 1
        return self.next_send - 1

    def start(self, src, dst, axis, to, index=None, send=None):
        if index is None:
            index = self.recv_index()
        kept = send is None
        if kept:
            send = self.send_index()
        copy = pltpu.make_async_remote_copy(
            src_ref=src,
            dst_ref=dst,
            send_sem=self.send_sems.at[send],
            recv_sem=self.recv_sems.at[index],
            device_id={AX[axis]: to},
            device_id_type=MESH,
        )
        copy.start()
        if kept:
            self.open.append(copy)
        return index

    def handle(self, ref, send, index, axis, peer):
        return pltpu.make_async_remote_copy(
            src_ref=ref,
            dst_ref=ref,
            send_sem=self.send_sems.at[send],
            recv_sem=self.recv_sems.at[index],
            device_id={AX[axis]: peer},
            device_id_type=MESH,
        )

    def wait(self, ref, index, axis, peer):
        self.handle(ref, 0, index, axis, peer).wait_recv()

    def wait_sent(self, ref, send, axis, peer):
        self.handle(ref, send, 0, axis, peer).wait_send()

    def drain(self):
        for copy in self.open:
            copy.wait_send()
        self.next_send -= len(self.open)
        self.open = []


def ring_relay(comm, me, n, axis, slot, arrived):
    size, s = n[axis], me[axis]
    at = lambda d: around(s, d, size)
    send = comm.send_index()
    near, far = comm.recv_index(), {1: comm.recv_index(), -1: comm.recv_index()}
    own = slot(s, None)
    for way in (1, -1):
        comm.start(own, own, axis, at(2 * way), far[way], send)
    for way in (1, -1):
        comm.start(own, own, axis, at(way), near, send)
    yield
    for way in (1, -1):
        piece = slot(at(-2 * way), None)
        comm.wait(piece, far[way], axis, at(-2 * way))
        comm.start(piece, piece, axis, at(way), near, send)
        half = slot(at(-2 * way), 0 if way > 0 else 1)
        comm.start(half, half, axis, at(2 * way), near, send)
    yield
    arrived(near, send)


def tree(comm, me, n, a1, a2, slot, arrived):
    n1, n2 = n[a1], (n[a2] if a2 else 1)
    s1, s2 = me[a1], (me[a2] if a2 else 0)
    held = {}

    def ref(d1, d2, h):
        return slot(around(s1, d1, n1), around(s2, d2, n2), h)

    def send(level, d1, d2, hop, way):
        axis, size, s = (a1, n1, s1) if level == 1 else (a2, n2, s2)
        half = None if hop < size // 2 else (0 if way > 0 else 1)
        piece = ref(d1, d2, half)
        index = comm.start(piece, piece, axis, around(s, way, size))
        key = (1, d1 - way, d2, hop, way) if level == 1 else (2, d1, d2 - way, hop, way)
        held[key] = (index, half)

    def take(level, d1, d2, hop, way):
        index, half = held.pop((level, d1, d2, hop, way))
        axis, size, s = (a1, n1, s1) if level == 1 else (a2, n2, s2)
        comm.wait(ref(d1, d2, half), index, axis, around(s, way, size))

    def spread(d1):
        if n2 > 1:
            for way in (1, -1):
                send(2, d1, 0, 1, way)

    if n1 > 1:
        for way in (1, -1):
            send(1, 0, 0, 1, way)
    spread(0)
    arrived(0, 0)
    yield
    last1, last2 = n1 // 2, n2 // 2
    for hop in range(1, last1 + last2 + 1):
        if n1 > 1 and hop <= last1:
            for way in (1, -1):
                d1 = -hop * way
                take(1, d1, 0, hop, way)
                if hop < last1:
                    send(1, d1, 0, hop + 1, way)
                    spread(d1)
                    arrived(d1, 0)
            if hop == last1:
                spread(last1)
                arrived(last1, 0)
        for t1 in range(last1 + 1):
            t2 = hop - t1
            if n2 == 1 or not 1 <= t2 <= last2:
                continue
            for d1 in [0] if t1 == 0 else [last1] if t1 == last1 else [-t1, t1]:
                for way in (1, -1):
                    d2 = -t2 * way
                    take(2, d1, d2, t2, way)
                    if t2 < last2:
                        send(2, d1, d2, t2 + 1, way)
                        arrived(d1, d2)
                if t2 == last2:
                    arrived(d1, last2)
        yield


def together(*walks):
    walks = list(walks)
    while walks:
        for walk in list(walks):
            try:
                next(walk)
            except StopIteration:
                walks.remove(walk)


def kernel(
    n, gain, x_ref, o_ref, xc, part, z1, x1, z2, x2, gram, cube, sums, rpg, cpg, rp2, cp2, rpp, cpp, rph, cps, rpn, cpw,
    qi, product, swap, edge, peaks, send_sems, recv_sems, local_sem,
):
    nz, nx, nc, ny = n["z"], n["x"], n["c"], n["y"]
    me = {a: (lax.axis_index(AX[a]) if n[a] > 1 else 0) for a in "zxcy"}
    z, x, c, y = me["z"], me["x"], me["c"], me["y"]
    rows_block, columns = x_ref.shape
    rows_half = rows_block // nc
    ph, pw = gram.shape
    half_rows = ph // 2
    mine = (y * nc + c) * nx + x
    comm = Comm(send_sems, recv_sems)

    barrier = pltpu.get_barrier_semaphore()
    peers = [(a, d) for a in "zxcy" for d in range(1, n[a])]
    for a, d in peers:
        pl.semaphore_signal(barrier, inc=1, device_id={AX[a]: around(me[a], d, n[a])}, device_id_type=MESH)
    pl.semaphore_wait(barrier, len(peers))

    parts = 2
    share = rows_block // parts

    def x_slot(i, q, h):
        if h is None:
            return xc.at[c, i, pl.ds(q * share, share)]
        return xc.at[c, i, pl.ds(q * share + h * (share // 2), share // 2)]

    own = pltpu.make_async_copy(x_ref, xc.at[c, y], local_sem)
    own.start()
    own.wait()
    to_partner = {}

    def x_arrived(q):
        def done(d, _):
            if nc > 1:
                ref = x_slot(around(y, d, ny), q, None)
                to_partner[q, d % ny] = comm.start(ref, ref, "c", 1 - c)

        return done

    together(*(tree(comm, me, n, "y", None, lambda i, _, h, q=q: x_slot(i, q, h), x_arrived(q)) for q in range(parts)))
    for (q, d), index in to_partner.items():
        comm.wait(xc.at[1 - c, around(y, d, ny), pl.ds(q * share, share)], index, "c", 1 - c)
    comm.drain()

    per_block = rows_block // pw
    top = pl.multiple_of(c * rows_half, rows_half)

    def right_rows(h, d):
        return xc[h, d // per_block, pl.ds(pl.multiple_of(d % per_block * pw, pw), pw)]

    def outer(left, right):
        return lax.dot_general(left, right, (((1,), (1,)), ((), ())), preferred_element_type=F32)

    def part_columns(d):
        total = sum(outer(xc[h, y, pl.ds(top, rows_half)], right_rows(h, d)) for h in range(nc))
        part[d] = total.astype(BF).reshape(nx, ph, pw)

    def part_rows(d):
        rows = pl.ds(pl.multiple_of(top + d * ph, ph), ph)

        def step(k, carry):
            part[k, d] = sum(outer(xc[h, y, rows], right_rows(h, k)) for h in range(nc)).astype(BF)
            return carry

        lax.fori_loop(0, nz, step, 0)

    def plus(piece, *more):
        total = piece[...].astype(F32)
        for other in more:
            total += other[...].astype(F32)
        return total

    def plane_sum(axis, piece, landing, chunks, prepare, across, final_landing):
        size, s = n[axis], me[axis]
        last = size // 2
        halves = {1: chunks[: len(chunks) // 2], -1: chunks[len(chunks) // 2 :]}
        index = {}
        send, final_send, final = comm.send_index(), comm.send_index(), comm.recv_index()

        def go(way, hop, e):
            index[way, hop, e] = comm.recv_index()
            d = around(s, way * (last - hop + 1), size)
            comm.start(piece(d, e), landing(way, hop, e), axis, around(s, way, size), index[way, hop, e], send)

        def come(way, hop, e):
            comm.wait(landing(way, hop, e), index[way, hop, e], axis, around(s, -way, size))
            return landing(way, hop, e)

        prepare(around(s, last, size))
        for a, b in zip(halves[1], halves[-1]):
            go(1, 1, a)
            go(-1, 1, b)
        for hop in range(2, last + 1):
            for way in (1, -1):
                prepare(around(s, way * (last - hop + 1), size))
                if hop == 2:
                    for e in halves[-way]:
                        go(way, hop, e)
            for k in range(len(chunks)):
                for way in (1, -1):
                    order = halves[way] if hop == 2 else halves[-way] + halves[way]
                    if k < len(order):
                        e = order[k]
                        ref = piece(around(s, way * (last - hop + 1), size), e)
                        ref[...] = plus(ref, come(way, hop - 1, e)).astype(BF)
                        go(way, hop, e)
        prepare(s)
        order = [e for pair in zip(halves[1], halves[-1]) for e in pair]
        for e in order:
            ref = piece(s, e)
            total = plus(ref, come(1, last, e), come(-1, last, e))
            if e == 0:
                gram[...] = total
            else:
                ref[...] = total.astype(BF)
                comm.start(ref, final_landing.at[e - 1], across, around(me[across], e, n[across]), final, final_send)
        comm.wait(final_landing, final, across, around(me[across], 1, n[across]))
        gram[...] = plus(gram, *(final_landing.at[k] for k in range(n[across] - 1)))
        comm.wait_sent(blocks((size - 1) * len(chunks)), send, axis, around(s, 1, size))
        comm.wait_sent(final_landing, final_send, across, around(me[across], 1, n[across]))

    def two_halves(ref, h, length):
        return ref if h is None else ref.at[pl.ds(h * length, length)]

    def blocks(count):
        across = next(k for k in range(nx, 0, -1) if count % k == 0 and count // k <= nz)
        return part.at[pl.ds(0, count // across), pl.ds(0, across)]

    base_recv, base_send = comm.next_recv, comm.next_send
    for core in range(nc):

        @pl.when(c == core)
        def _():
            comm.next_recv, comm.next_send = base_recv, base_send
            if core == 0:
                plane_sum(
                    "z", lambda d, e: part.at[d, around(x, e, nx)], lambda way, hop, e: z1.at[int(way > 0), hop - 1, e],
                    [2, 1, 3, 0], part_columns, "x", x2,
                )
            else:
                plane_sum(
                    "x", lambda d, e: part.at[around(z, e, nz), d], lambda way, hop, e: x1.at[int(way > 0), hop - 1, e],
                    [4, 5, 2, 7, 3, 6, 1, 0], part_rows, "z", z2,
                )

    comm.next_recv = comm.most_recv

    unsent = []

    def panels(rp, cp, half_done, peak=False):
        base_recv, base_send = comm.next_recv, comm.next_send
        for core in range(nc):

            @pl.when(c == core)
            def _():
                comm.next_recv, comm.next_send = base_recv, base_send
                over, peak_over = comm.recv_index(), comm.recv_index()
                send, send_over = comm.send_index(), comm.send_index()
                a1, a2 = ("y", "x") if core == 0 else ("x", "y")
                n1, n2 = n[a1], n[a2]
                at1, at2 = (lambda d: around(me[a1], d, n1)), (lambda d: around(me[a2], d, n2))

                def spot(d1, d2, h=None):
                    iy, ix = (at1(d1), at2(d2)) if a1 == "y" else (at2(d2), at1(d1))
                    return cp.at[iy, core, ix] if h is None else cp.at[iy, core, ix, pl.ds(h * half_rows, half_rows)]

                def group(d2):
                    return cp.at[:, core, at2(d2)] if a1 == "y" else cp.at[at2(d2), core]

                def to_partner(d2):
                    comm.start(group(d2), group(d2), "c", 1 - c, over, send_over)

                near1, far1, last = comm.recv_index(), comm.recv_index(), comm.recv_index()
                hop2 = {(way, k): comm.recv_index() for way in (1, -1) for k in range(3)}

                def spread(d1, k):
                    for way in (1, -1):
                        comm.start(spot(d1, 0), spot(d1, 0), a2, at2(way), hop2[way, k], send)
                    if d1 == 2:
                        comm.start(spot(d1, 0), spot(d1, 0), a2, at2(2), last, send)

                def pass_on(way, d1s):
                    for d1 in d1s:
                        half = spot(d1, -way, 0 if way > 0 else 1)
                        comm.start(half, half, a2, at2(way), last, send)

                def several(count):
                    return blocks(count)

                z_left = []
                z_walk = ring_relay(
                    comm, me, n, "z", lambda i, h: two_halves(rp.at[i], h, half_rows), lambda *left: z_left.append(left)
                )
                own = spot(0, 0)
                comm.start(own, own, a1, at1(2), far1, send)
                for way in (1, -1):
                    comm.start(own, own, a1, at1(way), near1, send)
                next(z_walk)
                spread(0, 0)
                peak_walk = largest(peak_over) if peak else iter(())
                next(peak_walk, None)

                comm.wait(several(2), near1, a1, at1(1))
                spread(-1, 1)
                spread(1, 1)
                for way in (1, -1):
                    comm.wait(own, hop2[way, 0], a2, at2(way))
                    pass_on(way, [0])
                comm.wait(own, far1, a1, at1(2))
                spread(2, 2)
                to_partner(0)
                next(z_walk)
                next(peak_walk, None)
                for way in (1, -1):
                    comm.wait(several(2), hop2[way, 1], a2, at2(way))
                    pass_on(way, [-1, 1])
                for way in (1, -1):
                    comm.wait(own, hop2[way, 2], a2, at2(way))
                    to_partner(-way)
                next(peak_walk, None)
                next(z_walk, None)
                comm.wait(several(4), last, a2, at2(1))
                to_partner(2)
                ((near, z_send),) = z_left
                comm.wait(rp.at[pl.ds(0, nz - 3)], near, "z", around(z, 1, nz))
                next(peak_walk, None)
                half_done()
                comm.wait(several(16), over, "c", 1 - c)
                if core == 0:
                    unsent.append((7, z_send, "z"))
                    unsent.append((15, send, "y"))
                    unsent.append((16, send_over, "c"))

        comm.next_recv = comm.most_recv

    def largest(over):
        kept = edge[0]
        sends = []
        for axis, at in (("y", 1), ("x", 1 + ny), ("c", 1 + ny + nx)):
            edge[at] = kept
            index, send = over if axis == "c" else comm.recv_index(), comm.send_index()
            for d in range(1, n[axis]):
                comm.start(edge.at[at], edge.at[at + d], axis, around(me[axis], d, n[axis]), index, send)
            yield
            comm.wait(edge.at[pl.ds(at + 1, n[axis] - 1)], index, axis, around(me[axis], 1, n[axis]))
            comm.wait_sent(edge.at[pl.ds(at + 1, n[axis] - 1)], send, axis, around(me[axis], 1, n[axis]))
            for d in range(1, n[axis]):
                kept = jnp.maximum(kept, edge[at + d])
        peaks[...] = kept

    def put(value, rp, cp):
        value = value.astype(BF)
        if rp is not None:
            rp[z] = value
        if cp is not None:
            cp[y, c, x] = value

    def times(rps, cp, core=None, totals=None):
        def step(k, totals):
            at = k if core is None else k * nc + core
            right = cp[at // nc, at % nc].reshape(nx * ph, pw)
            return tuple(t + jnp.dot(rp[at], right, preferred_element_type=F32) for t, rp in zip(totals, rps))

        if totals is None:
            totals = tuple(jnp.zeros((ph, pw), F32) for _ in rps)
        return lax.fori_loop(0, nz if core is None else nz // nc, step, totals)

    def exchange_and_times(rp, cp, pairs, peak=False):
        def half_done():
            at = 0
            for rps, right in pairs:
                for total in times(rps, right, c):
                    sums[at] = total
                    at += 1

        panels(rp, cp, half_done, peak)
        results, at = [], 0
        for rps, right in pairs:
            results += times(rps, right, 1 - c, tuple(sums[at + k] for k in range(len(rps))))
            at += len(rps)
        return results

    def with_identity(value, row, column, scale):
        rows = lax.broadcasted_iota(jnp.int32, value.shape, 0) + row
        across = lax.broadcasted_iota(jnp.int32, value.shape, 1) + column
        return value + jnp.where(rows == across, scale, 0.0)

    put(gram[...], rpg, cpg)
    (square,) = exchange_and_times(rpg, cpg, [([rpg], cpg)])

    def sizes(k, total):
        return total + jnp.abs(rpg[k].astype(F32))

    row_sums = jnp.sum(lax.fori_loop(0, nz, sizes, jnp.zeros((ph, pw), F32)), axis=1, keepdims=True)
    edge[0] = jnp.broadcast_to(jnp.max(row_sums, axis=0, keepdims=True), edge.shape[1:])
    put(square, rp2, cp2)
    panels(rp2, cp2, lambda: None, peak=True)

    bound = jnp.max(jnp.max(peaks[...], axis=1, keepdims=True), axis=0, keepdims=True) + epsilon
    inverse = 1.0 / bound
    root = lax.rsqrt(bound)

    def mix(once, twice, row, column):
        value = second_coef * (once.astype(F32) * inverse) + third_coef * (twice.astype(F32) * inverse * inverse)
        return with_identity(value, row, column, first_coef)

    def mix_rows(k, carry):
        rpp[k] = mix(rpg[k], rp2[k], mine * ph, k * pw).astype(BF)
        return carry

    def mix_columns(k, carry):
        at = (k // (nc * nx), k // nx % nc, k % nx)
        cpp[at] = mix(cpg[at], cp2[at], k * ph, z * pw).astype(BF)
        return carry

    lax.fori_loop(0, nz, mix_rows, 0)
    lax.fori_loop(0, ny * nc * nx, mix_columns, 0)
    cube[...] = mix(gram[...], square, mine * ph, z * pw)

    once, twice = times([rpg, rpp], cpp)
    put(once * inverse, rph, None)
    put(twice, None, cps)
    next_gram, next_first = exchange_and_times(rph, cps, [([rph], cpp), ([rph], cps)])
    put(next_gram, rpn, None)
    put(next_first, None, cpw)
    (next_second,) = exchange_and_times(rpn, cpw, [([rpn], cpw)])
    whole = (gain * root) * (first_coef * cube[...] + second_coef * next_first + third_coef * next_second)
    qi[z, x] = whole.astype(BF)

    def share_of(d):
        k = around(z, d, nz)
        left = qi[k].reshape(rows_half, pw)
        for side in range(nc):
            product[side] += jnp.dot(left, right_rows(around(c, 1 - side, nc), k), preferred_element_type=F32)

    product[...] = jnp.zeros(product.shape, F32)
    base_recv, base_send = comm.next_recv, comm.next_send

    def q(d, e, h=None):
        ref = qi.at[around(z, d, nz), around(x, e, nx)]
        return two_halves(ref, h, half_rows)

    def to_z(d, e, way, index, send, h=None):
        comm.start(q(d, e, h), q(d, e, h), "z", around(z, way, nz), index, send)

    def to_x(d, e, way, index, send, h=None):
        comm.start(q(d, e, h), q(d, e, h), "x", around(x, way, nx), index, send)

    def take(count, index, axis):
        comm.wait(blocks(count), index, axis, around(me[axis], 1, n[axis]))

    def gather_z_first():
        z_send, x_send = comm.send_index(), comm.send_index()
        far, near, three, four = {w: comm.recv_index() for w in (1, -1)}, comm.recv_index(), comm.recv_index(), comm.recv_index()
        groups = {0: [0], 1: [-1, 1], 2: [-2, 2], 3: [-3, 3], 4: [4]}
        hop = {(g, w): comm.recv_index() for g in groups for w in (1, -1)}
        last = {g: comm.recv_index() for g in groups}

        def spread(g, ds):
            for d in ds:
                for w in (1, -1):
                    to_x(d, 0, w, hop[g, w], x_send)
                if g == 4:
                    to_x(d, 0, 2, last[g], x_send)

        def pass_on(g):
            for w in (1, -1):
                take(len(groups[g]), hop[g, w], "x")
                if g < 4:
                    for d in groups[g]:
                        to_x(d, -w, w, last[g], x_send, 0 if w > 0 else 1)

        def finish(g):
            take(len(groups[g]), last[g], "x")
            for d in groups[g]:
                share_of(d)

        for w in (1, -1):
            to_z(0, 0, 2 * w, far[w], z_send)
        for w in (1, -1):
            to_z(0, 0, w, near, z_send)
        spread(0, [0])
        for w in (1, -1):
            take(1, far[w], "z")
            to_z(-2 * w, 0, w, three, z_send)
            to_z(-2 * w, 0, 2 * w, four, z_send, 0 if w > 0 else 1)
            spread(2, [-2 * w])
        take(2, near, "z")
        spread(1, groups[1])
        pass_on(0)
        take(2, three, "z")
        spread(3, groups[3])
        take(1, four, "z")
        spread(4, [4])
        pass_on(2)
        pass_on(1)
        finish(0)
        pass_on(3)
        finish(2)
        finish(1)
        pass_on(4)
        finish(3)
        finish(4)
        take_sent(7, z_send, "z")
        take_sent(24, x_send, "x")

    def gather_x_first():
        x_send, z_send = comm.send_index(), comm.send_index()
        near_x, far_x = comm.recv_index(), comm.recv_index()
        groups = {0: [0], 1: [-1, 1]}
        chain = {(g, h, w): comm.recv_index() for g in groups for h in range(1, 4) for w in (1, -1)}
        chain.update({(g, 4, w): k for g in groups for k in [comm.recv_index()] for w in (1, -1)})
        far, near, three, four = {w: comm.recv_index() for w in (1, -1)}, comm.recv_index(), comm.recv_index(), comm.recv_index()

        def go(g, h):
            for w in (1, -1):
                if h > 1:
                    take(len(groups[g]), chain[g, h - 1, w], "z")
                for e in groups[g]:
                    to_z(-w * (h - 1), e, w, chain[g, h, w], z_send, None if h < 4 else 0 if w > 0 else 1)

        to_x(0, 0, 2, far_x, x_send)
        for w in (1, -1):
            to_x(0, 0, w, near_x, x_send)
        go(0, 1)
        take(2, near_x, "x")
        go(1, 1)
        take(1, far_x, "x")
        for w in (1, -1):
            to_z(0, 2, 2 * w, far[w], z_send)
        for w in (1, -1):
            to_z(0, 2, w, near, z_send)
        go(0, 2)
        share_of(0)
        go(1, 2)
        go(0, 3)
        for w in (1, -1):
            take(1, far[w], "z")
            to_z(-2 * w, 2, w, three, z_send)
            to_z(-2 * w, 2, 2 * w, four, z_send, 0 if w > 0 else 1)
        go(1, 3)
        take(2, near, "z")
        share_of(-1)
        share_of(1)
        go(0, 4)
        share_of(-2)
        share_of(2)
        go(1, 4)
        take(2, three, "z")
        share_of(-3)
        share_of(3)
        take(1, four, "z")
        take(1, chain[0, 4, 1], "z")
        take(2, chain[1, 4, 1], "z")
        share_of(4)
        take_sent(3, x_send, "x")
        take_sent(28, z_send, "z")

    def take_sent(count, send, axis):
        comm.wait_sent(blocks(count), send, axis, around(me[axis], 1, n[axis]))

    for core in range(nc):

        @pl.when(c == core)
        def _():
            comm.next_recv, comm.next_send = base_recv, base_send
            (gather_z_first if core == 0 else gather_x_first)()

    comm.next_recv = comm.most_recv
    swap[0] = product[0].astype(BF)
    index = comm.start(swap.at[0], swap.at[1], "c", 1 - c)
    o_ref[pl.ds(top, rows_half)] = product[1].astype(BF)
    comm.wait(swap.at[1], index, "c", 1 - c)
    o_ref[pl.ds(pl.multiple_of((1 - c) * rows_half, rows_half), rows_half)] = swap[1]
    comm.drain()
    for count, send, axis in unsent:
        comm.wait_sent(rpg.at[pl.ds(0, count)] if count < nz else blocks(count), send, axis, around(me[axis], 1, n[axis]))


def update_call(n, gain, x):
    nz, nx, nc, ny = n["z"], n["x"], n["c"], n["y"]
    rows_block, columns = x.shape
    rows = rows_block * ny
    ph, pw = rows // (ny * nc * nx), rows // nz
    row_panel = pltpu.VMEM((nz, ph, pw), BF)
    column_panel = pltpu.VMEM((ny, nc, nx, ph, pw), BF)
    hops_z, hops_x = max(nz // 2, 1), max(nx // 2, 1)
    tiles = 2 + ny + nx + nc
    return pl.pallas_call(
        lambda *refs: kernel(n, gain, *refs),
        out_shape=jax.ShapeDtypeStruct(x.shape, BF),
        in_specs=[pl.BlockSpec(memory_space=pltpu.VMEM)],
        out_specs=pl.BlockSpec(memory_space=pltpu.VMEM),
        scratch_shapes=[
            pltpu.VMEM((nc, ny, rows_block, columns), BF),
            pltpu.VMEM((nz, nx, ph, pw), BF),
            pltpu.VMEM((2, hops_z, nx, ph, pw), BF),
            pltpu.VMEM((2, hops_x, nz, ph, pw), BF),
            pltpu.VMEM((nz - 1, ph, pw), BF),
            pltpu.VMEM((nx - 1, ph, pw), BF),
            pltpu.VMEM((ph, pw), F32),
            pltpu.VMEM((ph, pw), F32),
            pltpu.VMEM((2, ph, pw), F32),
            row_panel, column_panel, row_panel, column_panel, row_panel, column_panel,
            row_panel, column_panel, row_panel, column_panel,
            pltpu.VMEM((nz, nx, ph, pw), BF),
            pltpu.VMEM((nc, rows_block // nc, columns), F32),
            pltpu.VMEM((2, rows_block // nc, columns), BF),
            pltpu.VMEM((tiles, 8, 128), F32),
            pltpu.VMEM((8, 128), F32),
            pltpu.SemaphoreType.DMA((80,)),
            pltpu.SemaphoreType.DMA((300,)),
            pltpu.SemaphoreType.DMA,
        ],
        compiler_params=pltpu.CompilerParams(
            collective_id=0, has_side_effects=True, vmem_limit_bytes=48 * 1024 * 1024
        ),
    )(x)


def per_device(grad, momentum):
    new_momentum = momentum_beta * momentum + grad.astype(F32)
    iterate = (grad.astype(F32) + momentum_beta * new_momentum).astype(BF)
    update = update_call(SIZES, shape_gain * math.sqrt(max(R, C)), iterate)
    return (update, new_momentum)


def solution(mesh):
    devices = mesh.devices.reshape(SIZES["z"], SIZES["x"], SIZES["c"], SIZES["y"])
    split = Mesh(devices, (AX["z"], AX["x"], AX["c"], AX["y"]))
    mats = (AX["z"], AX["x"], AX["c"])
    return jax.shard_map(
        per_device,
        mesh=split,
        in_specs=(P(AX["y"], mats), P(AX["y"], mats)),
        out_specs=(P(AX["y"], mats), P(AX["y"], mats)),
        check_vma=False,
    )
```

```python
import math

import jax
import jax.numpy as jnp
from jax import lax
from jax.experimental import pallas as pl
from jax.experimental.pallas import tpu as pltpu
from jax.sharding import Mesh
from jax.sharding import PartitionSpec as P

R = 3072
C = 16384
AX = {"z": "mats_0", "x": "mats_1", "c": "mats_2", "y": "tp"}
SIZES = {"z": 8, "x": 4, "c": 2, "y": 4}

momentum_beta = 0.95
first_coef = 3.4445
second_coef = -4.775
third_coef = 2.0315
shape_gain = 0.2
epsilon = 1e-06

BF = jnp.bfloat16
F32 = jnp.float32
MESH = pl.DeviceIdType.MESH


def around(s, d, n):
    d = d % n
    return s if d == 0 else lax.rem(s + d, n)


class Comm:
    def __init__(self, send_sems, recv_sems):
        self.send_sems, self.recv_sems = send_sems, recv_sems
        self.next_send = self.next_recv = self.most_recv = 0
        self.open = []

    def recv_index(self):
        self.next_recv += 1
        self.most_recv = max(self.most_recv, self.next_recv)
        return self.next_recv - 1

    def send_index(self):
        self.next_send += 1
        return self.next_send - 1

    def start(self, src, dst, axis, to, index=None, send=None):
        if index is None:
            index = self.recv_index()
        kept = send is None
        if kept:
            send = self.send_index()
        copy = pltpu.make_async_remote_copy(
            src_ref=src,
            dst_ref=dst,
            send_sem=self.send_sems.at[send],
            recv_sem=self.recv_sems.at[index],
            device_id={AX[axis]: to},
            device_id_type=MESH,
        )
        copy.start()
        if kept:
            self.open.append(copy)
        return index

    def handle(self, ref, send, index, axis, peer):
        return pltpu.make_async_remote_copy(
            src_ref=ref,
            dst_ref=ref,
            send_sem=self.send_sems.at[send],
            recv_sem=self.recv_sems.at[index],
            device_id={AX[axis]: peer},
            device_id_type=MESH,
        )

    def wait(self, ref, index, axis, peer):
        self.handle(ref, 0, index, axis, peer).wait_recv()

    def wait_sent(self, ref, send, axis, peer):
        self.handle(ref, send, 0, axis, peer).wait_send()

    def drain(self):
        for copy in self.open:
            copy.wait_send()
        self.next_send -= len(self.open)
        self.open = []


def kernel(
    n, gain, x_ref, o_ref, xc, part, z1, x1, z2, x2, gram, cube, sums, rpg, cpg, rp2, cp2, rp3, cpp, rph, rpn, cpn, rpw,
    qi, product, swap, edge, peaks, send_sems, recv_sems, local_sem,
):
    nz, nx, nc, ny = n["z"], n["x"], n["c"], n["y"]
    me = {a: (lax.axis_index(AX[a]) if n[a] > 1 else 0) for a in "zxcy"}
    z, x, c, y = me["z"], me["x"], me["c"], me["y"]
    rows_block, columns = x_ref.shape
    rows_half = rows_block // nc
    ph, pw = gram.shape
    half_rows = ph // 2
    mine = (y * nc + c) * nx + x
    comm = Comm(send_sems, recv_sems)

    barrier = pltpu.get_barrier_semaphore()
    peers = [(a, d) for a in "zxcy" for d in range(1, n[a]) if a != "z" or d in (1, 2, nz - 2, nz - 1)]
    for a, d in peers:
        pl.semaphore_signal(barrier, inc=1, device_id={AX[a]: around(me[a], d, n[a])}, device_id_type=MESH)
    pl.semaphore_wait(barrier, len(peers))

    own = pltpu.make_async_copy(x_ref, xc.at[c, y], local_sem)
    own.start()
    quarter = rows_block // 4
    x_send, x_over_send, x_over = comm.send_index(), comm.send_index(), comm.recv_index()
    came = {(w, k): comm.recv_index() for w in (1, -1) for k in range(5)}

    def block(d, k, count=1):
        return xc.at[c, around(y, d, ny), pl.ds(k * quarter, count * quarter)]

    def to_y(ref, dst, w, k):
        comm.start(ref, dst, "y", around(y, w, ny), came[w, k], x_send)

    def from_y(w, k, ref):
        comm.wait(ref, came[w, k], "y", around(y, -w, ny))

    def to_other(d, k, count):
        comm.start(block(d, k, count), block(d, k, count), "c", 1 - c, x_over, x_over_send)

    for k in range(4):
        for w, q in ((1, k), (-1, 3 - k)):
            to_y(x_ref.at[pl.ds(q * quarter, quarter)], block(0, q), w, min(k, 2))
    comm.start(x_ref, xc.at[c, y], "c", 1 - c, x_over, x_over_send)
    for k in range(2):
        for w, q in ((1, k), (-1, 3 - k)):
            from_y(w, k, block(-w, q))
            to_y(block(-w, q), block(-w, q), w, 3 + k)
    to_other(-1, 0, 2)
    to_other(1, 2, 2)
    from_y(1, 2, block(-1, 2, 2))
    to_other(-1, 2, 2)
    from_y(-1, 2, block(1, 0, 2))
    to_other(1, 0, 2)
    for k in range(2):
        for w, q in ((1, k), (-1, 3 - k)):
            from_y(w, 3 + k, block(2, q))
            to_other(2, q, 1)
    own.wait()
    comm.wait(xc.at[1 - c], x_over, "c", 1 - c)
    comm.wait_sent(xc.at[c, pl.ds(0, 3)], x_send, "y", around(y, 1, ny))
    comm.wait_sent(xc.at[c], x_over_send, "c", 1 - c)

    per_block = rows_block // pw
    top = pl.multiple_of(c * rows_half, rows_half)

    def right_rows(h, d):
        return xc[h, d // per_block, pl.ds(pl.multiple_of(d % per_block * pw, pw), pw)]

    def outer(left, right):
        return lax.dot_general(left, right, (((1,), (1,)), ((), ())), preferred_element_type=F32)

    def part_columns(d):
        total = sum(outer(xc[h, y, pl.ds(top, rows_half)], right_rows(h, d)) for h in range(nc))
        part[d] = total.astype(BF).reshape(nx, ph, pw)

    def part_rows(d):
        rows = pl.ds(pl.multiple_of(top + d * ph, ph), ph)

        def step(k, carry):
            part[k, d] = sum(outer(xc[h, y, rows], right_rows(h, k)) for h in range(nc)).astype(BF)
            return carry

        lax.fori_loop(0, nz, step, 0)

    def plus(piece, *more):
        total = piece[...].astype(F32)
        for other in more:
            total += other[...].astype(F32)
        return total

    def plane_sum(axis, piece, landing, chunks, prepare, finish):
        size, s = n[axis], me[axis]
        last = size // 2
        halves = {1: chunks[: len(chunks) // 2], -1: chunks[len(chunks) // 2 :]}
        index = {}
        send = comm.send_index()

        def go(way, hop, e):
            index[way, hop, e] = comm.recv_index()
            d = around(s, way * (last - hop + 1), size)
            comm.start(piece(d, e), landing(way, hop, e), axis, around(s, way, size), index[way, hop, e], send)

        def come(way, hop, e):
            comm.wait(landing(way, hop, e), index[way, hop, e], axis, around(s, -way, size))
            return landing(way, hop, e)

        prepare(around(s, last, size))
        for a, b in zip(halves[1], halves[-1]):
            go(1, 1, a)
            go(-1, 1, b)
        for hop in range(2, last + 1):
            for way in (1, -1):
                prepare(around(s, way * (last - hop + 1), size))
                if hop == 2:
                    for e in halves[-way]:
                        go(way, hop, e)
            for k in range(len(chunks)):
                for way in (1, -1):
                    order = halves[way] if hop == 2 else halves[-way] + halves[way]
                    if k < len(order):
                        e = order[k]
                        ref = piece(around(s, way * (last - hop + 1), size), e)
                        ref[...] = plus(ref, come(way, hop - 1, e)).astype(BF)
                        go(way, hop, e)
        prepare(s)

        def summed(e):
            return plus(piece(s, e), come(1, last, e), come(-1, last, e))

        finish(summed, lambda e: piece(s, e))
        comm.wait_sent(blocks((size - 1) * len(chunks)), send, axis, around(s, 1, size))

    def straight_to_x(summed, kept):
        index, send = comm.recv_index(), comm.send_index()
        for e in (2, 3, 1, 0):
            if e == 0:
                gram[...] = summed(e)
            else:
                kept(e)[...] = summed(e).astype(BF)
                comm.start(kept(e), x2.at[e - 1], "x", around(x, e, nx), index, send)
        comm.wait(x2, index, "x", around(x, 1, nx))
        gram[...] = plus(gram, *(x2.at[k] for k in range(nx - 1)))
        comm.wait_sent(x2, send, "x", around(x, 1, nx))

    def two_hops_to_z(summed, kept):
        send, end = comm.send_index(), comm.recv_index()
        three = {w: comm.recv_index() for w in (1, -1)}
        four = {w: comm.recv_index() for w in (1, -1)}

        def go(ref, slot, index, way):
            comm.start(ref, slot, "z", around(z, way, nz), index, send)

        for e in (4, 3, 5, 6, 2, 1, 7):
            kept(e)[...] = summed(e).astype(BF)
            if e == 4:
                for w in (1, -1):
                    h = 0 if w > 0 else 1
                    go(two_halves(kept(4), h, half_rows), two_halves(z2.at[2], h, half_rows), four[w], 2 * w)
            elif e in (3, 5):
                w = 1 if e == 3 else -1
                go(kept(e), z2.at[0 if w > 0 else 1], three[w], w)
            elif e in (1, 7):
                w = 1 if e == 1 else -1
                go(kept(e), z2.at[3 if w > 0 else 4], end, w)
        gram[...] = summed(0)
        for w in (1, -1):
            mid = kept(2 * w % nz)
            slot, h = z2.at[0 if w > 0 else 1], 0 if w > 0 else 1
            comm.wait(slot, three[w], "z", around(z, -w, nz))
            mid[...] = plus(mid, slot).astype(BF)
            half = two_halves(z2.at[2], h, half_rows)
            comm.wait(half, four[w], "z", around(z, -2 * w, nz))
            part_of = two_halves(mid, h, half_rows)
            part_of[...] = plus(part_of, half).astype(BF)
            go(mid, z2.at[5 if w > 0 else 6], end, 2 * w)
        comm.wait(z2.at[pl.ds(3, 4)], end, "z", around(z, 1, nz))
        gram[...] = plus(gram, *(z2.at[k] for k in range(3, 7)))
        comm.wait_sent(z2, send, "z", around(z, 1, nz))

    def two_halves(ref, h, length):
        return ref if h is None else ref.at[pl.ds(h * length, length)]

    def blocks(count):
        across = next(k for k in range(nx, 0, -1) if count % k == 0 and count // k <= nz)
        return part.at[pl.ds(0, count // across), pl.ds(0, across)]

    base_recv, base_send = comm.next_recv, comm.next_send
    for core in range(nc):

        @pl.when(c == core)
        def _():
            comm.next_recv, comm.next_send = base_recv, base_send
            if core == 0:
                plane_sum(
                    "z", lambda d, e: part.at[d, around(x, e, nx)], lambda way, hop, e: z1.at[int(way > 0), hop - 1, e],
                    [2, 1, 3, 0], part_columns, straight_to_x,
                )
            else:
                plane_sum(
                    "x", lambda d, e: part.at[around(z, e, nz), d], lambda way, hop, e: x1.at[int(way > 0), hop - 1, e],
                    [4, 5, 2, 7, 3, 6, 1, 0], part_rows, two_hops_to_z,
                )

    comm.next_recv = comm.most_recv

    unsent = []

    def take(count, index, axis):
        comm.wait(blocks(count), index, axis, around(me[axis], 1, n[axis]))

    class Rows:
        def __init__(self, rp):
            self.rp, self.send = rp, comm.send_index()
            self.near, self.far = comm.recv_index(), {w: comm.recv_index() for w in (1, -1)}

        def to(self, d, way, index, h=None):
            ref = two_halves(self.rp.at[around(z, d, nz)], h, half_rows)
            comm.start(ref, ref, "z", around(z, way, nz), index, self.send)

        def begin(self):
            for w in (1, -1):
                self.to(0, 2 * w, self.far[w])
            for w in (1, -1):
                self.to(0, w, self.near)

        def forward(self):
            for w in (1, -1):
                take(1, self.far[w], "z")
                self.to(-2 * w, w, self.near)
                self.to(-2 * w, 2 * w, self.near, 0 if w > 0 else 1)

        def finish(self):
            take(nz - 3, self.near, "z")

    class Columns:
        def __init__(self, core, cp):
            self.core, self.cp = core, cp
            self.a1, self.a2 = ("y", "x") if core == 0 else ("x", "y")
            self.over, self.send_over, self.send = comm.recv_index(), comm.send_index(), comm.send_index()
            self.near, self.far, self.last = comm.recv_index(), comm.recv_index(), comm.recv_index()
            self.hop = {(w, k): comm.recv_index() for w in (1, -1) for k in range(3)}

        def at1(self, d):
            return around(me[self.a1], d, n[self.a1])

        def at2(self, d):
            return around(me[self.a2], d, n[self.a2])

        def spot(self, d1, d2, h=None):
            iy, ix = (self.at1(d1), self.at2(d2)) if self.a1 == "y" else (self.at2(d2), self.at1(d1))
            return two_halves(self.cp.at[iy, self.core, ix], h, half_rows)

        def to_partner(self, d2):
            ref = self.cp.at[:, self.core, self.at2(d2)] if self.a1 == "y" else self.cp.at[self.at2(d2), self.core]
            comm.start(ref, ref, "c", 1 - c, self.over, self.send_over)

        def spread(self, d1, k):
            ref = self.spot(d1, 0)
            for w in (1, -1):
                comm.start(ref, ref, self.a2, self.at2(w), self.hop[w, k], self.send)
            if d1 == 2:
                comm.start(ref, ref, self.a2, self.at2(2), self.last, self.send)

        def pass_on(self, w, d1s):
            for d1 in d1s:
                half = self.spot(d1, -w, 0 if w > 0 else 1)
                comm.start(half, half, self.a2, self.at2(w), self.last, self.send)

        def begin(self):
            own = self.spot(0, 0)
            comm.start(own, own, self.a1, self.at1(2), self.far, self.send)
            for w in (1, -1):
                comm.start(own, own, self.a1, self.at1(w), self.near, self.send)

        def first(self):
            take(2, self.near, self.a1)
            self.spread(-1, 1)
            self.spread(1, 1)
            for w in (1, -1):
                take(1, self.hop[w, 0], self.a2)
                self.pass_on(w, [0])
            take(1, self.far, self.a1)
            self.spread(2, 2)
            self.to_partner(0)

        def middle(self):
            for w in (1, -1):
                take(2, self.hop[w, 1], self.a2)
                self.pass_on(w, [-1, 1])
            for w in (1, -1):
                take(1, self.hop[w, 2], self.a2)
                self.to_partner(-w)

        def end(self):
            take(4, self.last, self.a2)
            self.to_partner(2)

        def finish(self):
            take(16, self.over, "c")

    def exchange(rp, cp, half_done=None, rp_next=None, next_piece=None, meanwhile=None, peak=False):
        base_recv, base_send = comm.next_recv, comm.next_send
        for core in range(nc):

            @pl.when(c == core)
            def _():
                comm.next_recv, comm.next_send = base_recv, base_send
                columns, rows = Columns(core, cp), Rows(rp)
                peak_walk = largest(comm.recv_index()) if peak else iter(())
                columns.begin()
                rows.begin()
                columns.spread(0, 0)
                next(peak_walk, None)
                if rp_next is None:
                    columns.first()
                    rows.forward()
                    columns.middle()
                    rows.finish()
                    columns.end()
                    half_done()
                    columns.finish()
                else:
                    rows.forward()
                    columns.first()
                    next(peak_walk, None)
                    rows.finish()
                    rp_next[z] = next_piece().astype(BF)
                    next_rows = Rows(rp_next)
                    next_rows.begin()
                    columns.middle()
                    next(peak_walk, None)
                    next_rows.forward()
                    columns.end()
                    next(peak_walk, None)
                    columns.finish()
                    meanwhile()
                    next_rows.finish()
                if core == 0:
                    unsent.append((7, rows.send, "z"))
                    unsent.append((15, columns.send, "y"))
                    unsent.append((16, columns.send_over, "c"))
                    if rp_next is not None:
                        unsent.append((7, next_rows.send, "z"))

        comm.next_recv = comm.most_recv

    def largest(over):
        kept = edge[0]
        sends = []
        for axis, at in (("y", 1), ("x", 1 + ny), ("c", 1 + ny + nx)):
            edge[at] = kept
            index, send = over if axis == "c" else comm.recv_index(), comm.send_index()
            for d in range(1, n[axis]):
                comm.start(edge.at[at], edge.at[at + d], axis, around(me[axis], d, n[axis]), index, send)
            yield
            comm.wait(edge.at[pl.ds(at + 1, n[axis] - 1)], index, axis, around(me[axis], 1, n[axis]))
            comm.wait_sent(edge.at[pl.ds(at + 1, n[axis] - 1)], send, axis, around(me[axis], 1, n[axis]))
            for d in range(1, n[axis]):
                kept = jnp.maximum(kept, edge[at + d])
        peaks[...] = kept

    def put(value, rp, cp):
        value = value.astype(BF)
        if rp is not None:
            rp[z] = value
        if cp is not None:
            cp[y, c, x] = value

    def times(rps, cp, core=None, totals=None):
        def step(k, totals):
            at = k if core is None else k * nc + core
            right = cp[at // nc, at % nc].reshape(nx * ph, pw)
            return tuple(t + jnp.dot(rp[at], right, preferred_element_type=F32) for t, rp in zip(totals, rps))

        if totals is None:
            totals = tuple(jnp.zeros((ph, pw), F32) for _ in rps)
        return lax.fori_loop(0, nz if core is None else nz // nc, step, totals)

    def with_identity(value, row, column, scale):
        rows = lax.broadcasted_iota(jnp.int32, value.shape, 0) + row
        across = lax.broadcasted_iota(jnp.int32, value.shape, 1) + column
        return value + jnp.where(rows == across, scale, 0.0)

    put(gram[...], rpg, cpg)

    def first_half():
        (sums[...],) = times([rpg], cpg, c)

    exchange(rpg, cpg, first_half)

    def sizes(k, total):
        return total + jnp.abs(rpg[k].astype(F32))

    row_sums = jnp.sum(lax.fori_loop(0, nz, sizes, jnp.zeros((ph, pw), F32)), axis=1, keepdims=True)
    edge[0] = jnp.broadcast_to(jnp.max(row_sums, axis=0, keepdims=True), edge.shape[1:])
    (square,) = times([rpg], cpg, 1 - c, (sums[...],))
    sums[...] = square
    put(square, rp2, cp2)

    def scales():
        bound = jnp.max(jnp.max(peaks[...], axis=1, keepdims=True), axis=0, keepdims=True) + epsilon
        return 1.0 / bound, lax.rsqrt(bound)

    def mix(once, twice, inverse, row, column):
        value = second_coef * (once.astype(F32) * inverse) + third_coef * (twice.astype(F32) * inverse * inverse)
        return with_identity(value, row, column, first_coef)

    def mixed_columns():
        inverse, _ = scales()

        def step(k, carry):
            at = (k // (nc * nx), k // nx % nc, k % nx)
            cpp[at] = mix(cpg[at], cp2[at], inverse, k * ph, z * pw).astype(BF)
            return carry

        lax.fori_loop(0, ny * nc * nx, step, 0)
        cube[...] = mix(gram[...], sums[...], inverse, mine * ph, z * pw)

    exchange(rp2, cp2, None, rp3, lambda: times([rp2], cpg)[0], mixed_columns, peak=True)

    inverse, root = scales()

    def product_rows(k, carry):
        once = rpg[k].astype(F32) * inverse
        twice = rp2[k].astype(F32) * inverse * inverse
        thrice = rp3[k].astype(F32) * inverse * inverse * inverse
        rph[k] = (first_coef * once + second_coef * twice + third_coef * thrice).astype(BF)
        return carry

    lax.fori_loop(0, nz, product_rows, 0)
    (next_gram,) = times([rph], cpp)
    put(next_gram, rpn, cpn)

    def next_first():
        (value,) = times([rpn], cpp)
        sums[...] = value
        return value

    exchange(rpn, cpn, None, rpw, next_first, lambda: None)
    (next_second,) = times([rpw], cpn)
    whole = (gain * root) * (first_coef * cube[...] + second_coef * sums[...] + third_coef * next_second)
    qi[z, x] = whole.astype(BF)

    def share_of(d):
        k = around(z, d, nz)
        left = qi[k].reshape(rows_half, pw)
        for side in range(nc):
            product[side] += jnp.dot(left, right_rows(around(c, 1 - side, nc), k), preferred_element_type=F32)

    product[...] = jnp.zeros(product.shape, F32)
    base_recv, base_send = comm.next_recv, comm.next_send

    def q(d, e, h=None):
        ref = qi.at[around(z, d, nz), around(x, e, nx)]
        return two_halves(ref, h, half_rows)

    def to_z(d, e, way, index, send, h=None):
        comm.start(q(d, e, h), q(d, e, h), "z", around(z, way, nz), index, send)

    def to_x(d, e, way, index, send, h=None):
        comm.start(q(d, e, h), q(d, e, h), "x", around(x, way, nx), index, send)

    def gather_z_first():
        z_send, x_send = comm.send_index(), comm.send_index()
        far, near, three, four = {w: comm.recv_index() for w in (1, -1)}, comm.recv_index(), comm.recv_index(), comm.recv_index()
        groups = {0: [0], 1: [-1, 1], 2: [-2, 2], 3: [-3, 3], 4: [4]}
        hop = {(g, w): comm.recv_index() for g in groups for w in (1, -1)}
        last = {g: comm.recv_index() for g in groups}

        def spread(g, ds):
            for d in ds:
                for w in (1, -1):
                    to_x(d, 0, w, hop[g, w], x_send)
                if g == 4:
                    to_x(d, 0, 2, last[g], x_send)

        def pass_on(g):
            for w in (1, -1):
                take(len(groups[g]), hop[g, w], "x")
                if g < 4:
                    for d in groups[g]:
                        to_x(d, -w, w, last[g], x_send, 0 if w > 0 else 1)

        def finish(g):
            take(len(groups[g]), last[g], "x")
            for d in groups[g]:
                share_of(d)

        for w in (1, -1):
            to_z(0, 0, 2 * w, far[w], z_send)
        for w in (1, -1):
            to_z(0, 0, w, near, z_send)
        spread(0, [0])
        for w in (1, -1):
            take(1, far[w], "z")
            to_z(-2 * w, 0, w, three, z_send)
            to_z(-2 * w, 0, 2 * w, four, z_send, 0 if w > 0 else 1)
            spread(2, [-2 * w])
        take(2, near, "z")
        spread(1, groups[1])
        pass_on(0)
        take(2, three, "z")
        spread(3, groups[3])
        take(1, four, "z")
        spread(4, [4])
        pass_on(2)
        pass_on(1)
        finish(0)
        pass_on(3)
        finish(2)
        finish(1)
        pass_on(4)
        finish(3)
        finish(4)
        take_sent(7, z_send, "z")
        take_sent(24, x_send, "x")

    def gather_x_first():
        x_send, z_send = comm.send_index(), comm.send_index()
        near_x, far_x = comm.recv_index(), comm.recv_index()
        groups = {0: [0], 1: [-1, 1]}
        chain = {(g, h, w): comm.recv_index() for g in groups for h in range(1, 4) for w in (1, -1)}
        chain.update({(g, 4, w): k for g in groups for k in [comm.recv_index()] for w in (1, -1)})
        far, near, three, four = {w: comm.recv_index() for w in (1, -1)}, comm.recv_index(), comm.recv_index(), comm.recv_index()

        def go(g, h):
            for w in (1, -1):
                if h > 1:
                    take(len(groups[g]), chain[g, h - 1, w], "z")
                for e in groups[g]:
                    to_z(-w * (h - 1), e, w, chain[g, h, w], z_send, None if h < 4 else 0 if w > 0 else 1)

        to_x(0, 0, 2, far_x, x_send)
        for w in (1, -1):
            to_x(0, 0, w, near_x, x_send)
        go(0, 1)
        take(2, near_x, "x")
        go(1, 1)
        take(1, far_x, "x")
        for w in (1, -1):
            to_z(0, 2, 2 * w, far[w], z_send)
        for w in (1, -1):
            to_z(0, 2, w, near, z_send)
        go(0, 2)
        share_of(0)
        go(1, 2)
        go(0, 3)
        for w in (1, -1):
            take(1, far[w], "z")
            to_z(-2 * w, 2, w, three, z_send)
            to_z(-2 * w, 2, 2 * w, four, z_send, 0 if w > 0 else 1)
        go(1, 3)
        take(2, near, "z")
        share_of(-1)
        share_of(1)
        go(0, 4)
        share_of(-2)
        share_of(2)
        go(1, 4)
        take(2, three, "z")
        share_of(-3)
        share_of(3)
        take(1, four, "z")
        take(1, chain[0, 4, 1], "z")
        take(2, chain[1, 4, 1], "z")
        share_of(4)
        take_sent(3, x_send, "x")
        take_sent(28, z_send, "z")

    def take_sent(count, send, axis):
        comm.wait_sent(blocks(count), send, axis, around(me[axis], 1, n[axis]))

    for core in range(nc):

        @pl.when(c == core)
        def _():
            comm.next_recv, comm.next_send = base_recv, base_send
            (gather_z_first if core == 0 else gather_x_first)()

    comm.next_recv = comm.most_recv
    swap[0] = product[0].astype(BF)
    index = comm.start(swap.at[0], swap.at[1], "c", 1 - c)
    o_ref[pl.ds(top, rows_half)] = product[1].astype(BF)
    comm.wait(swap.at[1], index, "c", 1 - c)
    o_ref[pl.ds(pl.multiple_of((1 - c) * rows_half, rows_half), rows_half)] = swap[1]
    comm.drain()
    for count, send, axis in unsent:
        comm.wait_sent(rpg.at[pl.ds(0, count)] if count < nz else blocks(count), send, axis, around(me[axis], 1, n[axis]))


def update_call(n, gain, x):
    nz, nx, nc, ny = n["z"], n["x"], n["c"], n["y"]
    rows_block, columns = x.shape
    rows = rows_block * ny
    ph, pw = rows // (ny * nc * nx), rows // nz
    row_panel = pltpu.VMEM((nz, ph, pw), BF)
    column_panel = pltpu.VMEM((ny, nc, nx, ph, pw), BF)
    hops_z, hops_x = max(nz // 2, 1), max(nx // 2, 1)
    tiles = 2 + ny + nx + nc
    return pl.pallas_call(
        lambda *refs: kernel(n, gain, *refs),
        out_shape=jax.ShapeDtypeStruct(x.shape, BF),
        in_specs=[pl.BlockSpec(memory_space=pltpu.VMEM)],
        out_specs=pl.BlockSpec(memory_space=pltpu.VMEM),
        scratch_shapes=[
            pltpu.VMEM((nc, ny, rows_block, columns), BF),
            pltpu.VMEM((nz, nx, ph, pw), BF),
            pltpu.VMEM((2, hops_z, nx, ph, pw), BF),
            pltpu.VMEM((2, hops_x, nz, ph, pw), BF),
            pltpu.VMEM((nz - 1, ph, pw), BF),
            pltpu.VMEM((nx - 1, ph, pw), BF),
            pltpu.VMEM((ph, pw), F32),
            pltpu.VMEM((ph, pw), F32),
            pltpu.VMEM((ph, pw), F32),
            row_panel, column_panel, row_panel, column_panel, row_panel, column_panel,
            row_panel, row_panel, column_panel, row_panel,
            pltpu.VMEM((nz, nx, ph, pw), BF),
            pltpu.VMEM((nc, rows_block // nc, columns), F32),
            pltpu.VMEM((2, rows_block // nc, columns), BF),
            pltpu.VMEM((tiles, 8, 128), F32),
            pltpu.VMEM((8, 128), F32),
            pltpu.SemaphoreType.DMA((80,)),
            pltpu.SemaphoreType.DMA((300,)),
            pltpu.SemaphoreType.DMA,
        ],
        compiler_params=pltpu.CompilerParams(
            collective_id=0, has_side_effects=True, vmem_limit_bytes=48 * 1024 * 1024
        ),
    )(x)


def per_device(grad, momentum):
    new_momentum = momentum_beta * momentum + grad.astype(F32)
    iterate = (grad.astype(F32) + momentum_beta * new_momentum).astype(BF)
    update = update_call(SIZES, shape_gain * math.sqrt(max(R, C)), iterate)
    return (update, new_momentum)


def solution(mesh):
    devices = mesh.devices.reshape(SIZES["z"], SIZES["x"], SIZES["c"], SIZES["y"])
    split = Mesh(devices, (AX["z"], AX["x"], AX["c"], AX["y"]))
    mats = (AX["z"], AX["x"], AX["c"])
    return jax.shard_map(
        per_device,
        mesh=split,
        in_specs=(P(AX["y"], mats), P(AX["y"], mats)),
        out_specs=(P(AX["y"], mats), P(AX["y"], mats)),
        check_vma=False,
    )
```

```python
import math

import jax
import jax.numpy as jnp
from jax import lax
from jax.experimental import pallas as pl
from jax.experimental.pallas import tpu as pltpu
from jax.sharding import Mesh
from jax.sharding import PartitionSpec as P

R = 3072
C = 16384
AX = {"z": "mats_0", "x": "mats_1", "c": "mats_2", "y": "tp"}
SIZES = {"z": 8, "x": 4, "c": 2, "y": 4}

momentum_beta = 0.95
first_coef = 3.4445
second_coef = -4.775
third_coef = 2.0315
shape_gain = 0.2
epsilon = 1e-06

BF = jnp.bfloat16
F32 = jnp.float32
MESH = pl.DeviceIdType.MESH


def around(s, d, n):
    d = d % n
    return s if d == 0 else lax.rem(s + d, n)


class Comm:
    def __init__(self, send_sems, recv_sems):
        self.send_sems, self.recv_sems = send_sems, recv_sems
        self.next_send = self.next_recv = self.most_recv = 0
        self.open = []

    def recv_index(self):
        self.next_recv += 1
        self.most_recv = max(self.most_recv, self.next_recv)
        return self.next_recv - 1

    def send_index(self):
        self.next_send += 1
        return self.next_send - 1

    def start(self, src, dst, axis, to, index=None, send=None):
        if index is None:
            index = self.recv_index()
        kept = send is None
        if kept:
            send = self.send_index()
        copy = pltpu.make_async_remote_copy(
            src_ref=src,
            dst_ref=dst,
            send_sem=self.send_sems.at[send],
            recv_sem=self.recv_sems.at[index],
            device_id={AX[axis]: to},
            device_id_type=MESH,
        )
        copy.start()
        if kept:
            self.open.append(copy)
        return index

    def handle(self, ref, send, index, axis, peer):
        return pltpu.make_async_remote_copy(
            src_ref=ref,
            dst_ref=ref,
            send_sem=self.send_sems.at[send],
            recv_sem=self.recv_sems.at[index],
            device_id={AX[axis]: peer},
            device_id_type=MESH,
        )

    def wait(self, ref, index, axis, peer):
        self.handle(ref, 0, index, axis, peer).wait_recv()

    def wait_sent(self, ref, send, axis, peer):
        self.handle(ref, send, 0, axis, peer).wait_send()

    def drain(self):
        for copy in self.open:
            copy.wait_send()
        self.next_send -= len(self.open)
        self.open = []


def kernel(
    n, gain, x_ref, o_ref, xc, part, z1, x1, z2, x2, gram, cube, sums, total_ref, rpg, cpg, rp2, cp2, rp3, cpp, rpn, cpn, rpw,
    qi, product, swap, edge, peaks, send_sems, recv_sems, local_sem,
):
    nz, nx, nc, ny = n["z"], n["x"], n["c"], n["y"]
    me = {a: (lax.axis_index(AX[a]) if n[a] > 1 else 0) for a in "zxcy"}
    z, x, c, y = me["z"], me["x"], me["c"], me["y"]
    rows_block, columns = x_ref.shape
    rows_half = rows_block // nc
    ph, pw = gram.shape
    half_rows = ph // 2
    mine = (y * nc + c) * nx + x
    comm = Comm(send_sems, recv_sems)

    barrier = pltpu.get_barrier_semaphore()
    peers = [(a, d) for a in "zxcy" for d in range(1, n[a]) if a != "z" or d in (1, 2, nz - 2, nz - 1)]
    for a, d in peers:
        pl.semaphore_signal(barrier, inc=1, device_id={AX[a]: around(me[a], d, n[a])}, device_id_type=MESH)
    pl.semaphore_wait(barrier, len(peers))

    own = pltpu.make_async_copy(x_ref, xc.at[c, y], local_sem)
    own.start()
    quarter = rows_block // 4
    x_send, x_over_send, x_over = comm.send_index(), comm.send_index(), comm.recv_index()
    came = {(w, k): comm.recv_index() for w in (1, -1) for k in range(5)}

    def block(d, k, count=1):
        return xc.at[c, around(y, d, ny), pl.ds(k * quarter, count * quarter)]

    def to_y(ref, dst, w, k):
        comm.start(ref, dst, "y", around(y, w, ny), came[w, k], x_send)

    def from_y(w, k, ref):
        comm.wait(ref, came[w, k], "y", around(y, -w, ny))

    def to_other(d, k, count):
        comm.start(block(d, k, count), block(d, k, count), "c", 1 - c, x_over, x_over_send)

    for k in range(4):
        for w, q in ((1, k), (-1, 3 - k)):
            to_y(x_ref.at[pl.ds(q * quarter, quarter)], block(0, q), w, min(k, 2))
    comm.start(x_ref, xc.at[c, y], "c", 1 - c, x_over, x_over_send)
    for k in range(2):
        for w, q in ((1, k), (-1, 3 - k)):
            from_y(w, k, block(-w, q))
            to_y(block(-w, q), block(-w, q), w, 3 + k)
    to_other(-1, 0, 2)
    to_other(1, 2, 2)
    from_y(1, 2, block(-1, 2, 2))
    to_other(-1, 2, 2)
    from_y(-1, 2, block(1, 0, 2))
    to_other(1, 0, 2)
    for k in range(2):
        for w, q in ((1, k), (-1, 3 - k)):
            from_y(w, 3 + k, block(2, q))
            to_other(2, q, 1)
    own.wait()
    comm.wait(xc.at[1 - c], x_over, "c", 1 - c)
    comm.wait_sent(xc.at[c, pl.ds(0, 3)], x_send, "y", around(y, 1, ny))
    comm.wait_sent(xc.at[c], x_over_send, "c", 1 - c)

    per_block = rows_block // pw
    top = pl.multiple_of(c * rows_half, rows_half)

    def right_rows(h, d):
        return xc[h, d // per_block, pl.ds(pl.multiple_of(d % per_block * pw, pw), pw)]

    def outer(left, right):
        return lax.dot_general(left, right, (((1,), (1,)), ((), ())), preferred_element_type=F32)

    def part_columns(d):
        total = sum(outer(xc[h, y, pl.ds(top, rows_half)], right_rows(h, d)) for h in range(nc))
        part[d] = total.astype(BF).reshape(nx, ph, pw)

    def part_rows(d):
        rows = pl.ds(pl.multiple_of(top + d * ph, ph), ph)

        def step(k, carry):
            part[k, d] = sum(outer(xc[h, y, rows], right_rows(h, k)) for h in range(nc)).astype(BF)
            return carry

        lax.fori_loop(0, nz, step, 0)

    def plus(piece, *more):
        total = piece[...].astype(F32)
        for other in more:
            total += other[...].astype(F32)
        return total

    def plane_sum(axis, piece, landing, chunks, prepare, finish):
        size, s = n[axis], me[axis]
        last = size // 2
        halves = {1: chunks[: len(chunks) // 2], -1: chunks[len(chunks) // 2 :]}
        index = {}
        send = comm.send_index()

        def go(way, hop, e):
            index[way, hop, e] = comm.recv_index()
            d = around(s, way * (last - hop + 1), size)
            comm.start(piece(d, e), landing(way, hop, e), axis, around(s, way, size), index[way, hop, e], send)

        def come(way, hop, e):
            comm.wait(landing(way, hop, e), index[way, hop, e], axis, around(s, -way, size))
            return landing(way, hop, e)

        prepare(around(s, last, size))
        for a, b in zip(halves[1], halves[-1]):
            go(1, 1, a)
            go(-1, 1, b)
        for hop in range(2, last + 1):
            for way in (1, -1):
                prepare(around(s, way * (last - hop + 1), size))
                if hop == 2:
                    for e in halves[-way]:
                        go(way, hop, e)
            for k in range(len(chunks)):
                for way in (1, -1):
                    order = halves[way] if hop == 2 else halves[-way] + halves[way]
                    if k < len(order):
                        e = order[k]
                        ref = piece(around(s, way * (last - hop + 1), size), e)
                        ref[...] = plus(ref, come(way, hop - 1, e)).astype(BF)
                        go(way, hop, e)
        prepare(s)

        def summed(e):
            return plus(piece(s, e), come(1, last, e), come(-1, last, e))

        finish(summed, lambda e: piece(s, e))
        comm.wait_sent(blocks((size - 1) * len(chunks)), send, axis, around(s, 1, size))

    def straight_to_x(summed, kept):
        index, send = comm.recv_index(), comm.send_index()
        for e in (2, 3, 1, 0):
            if e == 0:
                gram[...] = summed(e)
            else:
                kept(e)[...] = summed(e).astype(BF)
                comm.start(kept(e), x2.at[e - 1], "x", around(x, e, nx), index, send)
        comm.wait(x2, index, "x", around(x, 1, nx))
        gram[...] = plus(gram, *(x2.at[k] for k in range(nx - 1)))
        comm.wait_sent(x2, send, "x", around(x, 1, nx))

    def two_hops_to_z(summed, kept):
        send, end = comm.send_index(), comm.recv_index()
        three = {w: comm.recv_index() for w in (1, -1)}
        four = {w: comm.recv_index() for w in (1, -1)}

        def go(ref, slot, index, way):
            comm.start(ref, slot, "z", around(z, way, nz), index, send)

        for e in (4, 3, 5, 6, 2, 1, 7):
            kept(e)[...] = summed(e).astype(BF)
            if e == 4:
                for w in (1, -1):
                    h = 0 if w > 0 else 1
                    go(two_halves(kept(4), h, half_rows), two_halves(z2.at[2], h, half_rows), four[w], 2 * w)
            elif e in (3, 5):
                w = 1 if e == 3 else -1
                go(kept(e), z2.at[0 if w > 0 else 1], three[w], w)
            elif e in (1, 7):
                w = 1 if e == 1 else -1
                go(kept(e), z2.at[3 if w > 0 else 4], end, w)
        gram[...] = summed(0)
        for w in (1, -1):
            mid = kept(2 * w % nz)
            slot, h = z2.at[0 if w > 0 else 1], 0 if w > 0 else 1
            comm.wait(slot, three[w], "z", around(z, -w, nz))
            mid[...] = plus(mid, slot).astype(BF)
            half = two_halves(z2.at[2], h, half_rows)
            comm.wait(half, four[w], "z", around(z, -2 * w, nz))
            part_of = two_halves(mid, h, half_rows)
            part_of[...] = plus(part_of, half).astype(BF)
            go(mid, z2.at[5 if w > 0 else 6], end, 2 * w)
        comm.wait(z2.at[pl.ds(3, 4)], end, "z", around(z, 1, nz))
        gram[...] = plus(gram, *(z2.at[k] for k in range(3, 7)))
        comm.wait_sent(z2, send, "z", around(z, 1, nz))

    def two_halves(ref, h, length):
        return ref if h is None else ref.at[pl.ds(h * length, length)]

    def blocks(count):
        across = next(k for k in range(nx, 0, -1) if count % k == 0 and count // k <= nz)
        return part.at[pl.ds(0, count // across), pl.ds(0, across)]

    base_recv, base_send = comm.next_recv, comm.next_send
    for core in range(nc):

        @pl.when(c == core)
        def _():
            comm.next_recv, comm.next_send = base_recv, base_send
            if core == 0:
                plane_sum(
                    "z", lambda d, e: part.at[d, around(x, e, nx)], lambda way, hop, e: z1.at[int(way > 0), hop - 1, e],
                    [2, 1, 3, 0], part_columns, straight_to_x,
                )
            else:
                plane_sum(
                    "x", lambda d, e: part.at[around(z, e, nz), d], lambda way, hop, e: x1.at[int(way > 0), hop - 1, e],
                    [4, 5, 2, 7, 3, 6, 1, 0], part_rows, two_hops_to_z,
                )

    comm.next_recv = comm.most_recv

    unsent = []

    def take(count, index, axis):
        comm.wait(blocks(count), index, axis, around(me[axis], 1, n[axis]))

    class Rows:
        def __init__(self, rp):
            self.rp, self.send = rp, comm.send_index()
            self.near, self.rest, self.far = comm.recv_index(), comm.recv_index(), {w: comm.recv_index() for w in (1, -1)}

        def to(self, d, way, index, h=None):
            ref = two_halves(self.rp.at[around(z, d, nz)], h, half_rows)
            comm.start(ref, ref, "z", around(z, way, nz), index, self.send)

        def begin(self):
            for w in (1, -1):
                self.to(0, 2 * w, self.far[w])
            for w in (1, -1):
                self.to(0, w, self.near)

        def forward(self):
            for w in (1, -1):
                take(1, self.far[w], "z")
                self.to(-2 * w, 2 * w, self.rest, 0 if w > 0 else 1)
                self.to(-2 * w, w, self.rest)

        def finish(self, use=lambda ds: None):
            use([-2, 2])
            take(2, self.near, "z")
            use([-1, 1])
            take(3, self.rest, "z")
            use([-3, 3, 4])

    class Columns:
        def __init__(self, core, cp):
            self.core, self.cp = core, cp
            self.a1, self.a2 = ("y", "x") if core == 0 else ("x", "y")
            self.over, self.send_over, self.send = comm.recv_index(), comm.send_index(), comm.send_index()
            self.near, self.far, self.last = comm.recv_index(), comm.recv_index(), comm.recv_index()
            self.hop = {(w, k): comm.recv_index() for w in (1, -1) for k in range(3)}

        def at1(self, d):
            return around(me[self.a1], d, n[self.a1])

        def at2(self, d):
            return around(me[self.a2], d, n[self.a2])

        def spot(self, d1, d2, h=None):
            iy, ix = (self.at1(d1), self.at2(d2)) if self.a1 == "y" else (self.at2(d2), self.at1(d1))
            return two_halves(self.cp.at[iy, self.core, ix], h, half_rows)

        def to_partner(self, d2):
            ref = self.cp.at[:, self.core, self.at2(d2)] if self.a1 == "y" else self.cp.at[self.at2(d2), self.core]
            comm.start(ref, ref, "c", 1 - c, self.over, self.send_over)

        def spread(self, d1, k):
            ref = self.spot(d1, 0)
            for w in (1, -1):
                comm.start(ref, ref, self.a2, self.at2(w), self.hop[w, k], self.send)
            if d1 == 2:
                comm.start(ref, ref, self.a2, self.at2(2), self.last, self.send)

        def pass_on(self, w, d1s):
            for d1 in d1s:
                half = self.spot(d1, -w, 0 if w > 0 else 1)
                comm.start(half, half, self.a2, self.at2(w), self.last, self.send)

        def begin(self):
            own = self.spot(0, 0)
            comm.start(own, own, self.a1, self.at1(2), self.far, self.send)
            for w in (1, -1):
                comm.start(own, own, self.a1, self.at1(w), self.near, self.send)

        def first(self):
            take(2, self.near, self.a1)
            self.spread(-1, 1)
            self.spread(1, 1)
            for w in (1, -1):
                take(1, self.hop[w, 0], self.a2)
                self.pass_on(w, [0])
            take(1, self.far, self.a1)
            self.spread(2, 2)
            self.to_partner(0)

        def middle(self):
            for w in (1, -1):
                take(2, self.hop[w, 1], self.a2)
                self.pass_on(w, [-1, 1])
            for w in (1, -1):
                take(1, self.hop[w, 2], self.a2)
                self.to_partner(-w)

        def end(self):
            take(4, self.last, self.a2)
            self.to_partner(2)

        def finish(self):
            take(16, self.over, "c")

    def gather_panels(rp, cp, half_done):
        base_recv, base_send = comm.next_recv, comm.next_send
        for core in range(nc):

            @pl.when(c == core)
            def _():
                comm.next_recv, comm.next_send = base_recv, base_send
                columns, rows = Columns(core, cp), Rows(rp)
                columns.begin()
                rows.begin()
                columns.spread(0, 0)
                columns.first()
                rows.forward()
                columns.middle()
                rows.finish()
                columns.end()
                half_done()
                columns.finish()
                if core == 0:
                    sent(columns, rows)

        comm.next_recv = comm.most_recv

    def sent(columns, *rows):
        unsent.append((15, columns.send, "y"))
        unsent.append((16, columns.send_over, "c"))
        unsent.extend((7, each.send, "z") for each in rows)

    def adding(left, cp):
        def use(ds):
            total = total_ref[...]
            for d in ds:
                k = around(z, d, nz)
                total += jnp.dot(left(k), cp[k // nc, k % nc].reshape(nx * ph, pw), preferred_element_type=F32)
            total_ref[...] = total

        return use

    def two_products(rp, cp, first, rp_next, next_piece, meanwhile, second, peak=False):
        base_recv, base_send = comm.next_recv, comm.next_send
        for core in range(nc):

            @pl.when(c == core)
            def _():
                comm.next_recv, comm.next_send = base_recv, base_send
                columns, rows = Columns(core, cp), Rows(rp)
                peak_walk = largest(comm.recv_index()) if peak else iter(())
                rows.begin()
                columns.begin()
                columns.spread(0, 0)
                next(peak_walk, None)
                total_ref[...] = jnp.zeros(total_ref.shape, F32)
                first([0])
                rows.forward()
                columns.first()
                next(peak_walk, None)
                rows.finish(first)
                rp_next[z] = next_piece(total_ref[...]).astype(BF)
                next_rows = Rows(rp_next)
                next_rows.begin()
                total_ref[...] = jnp.zeros(total_ref.shape, F32)
                columns.middle()
                next(peak_walk, None)
                next_rows.forward()
                columns.end()
                next(peak_walk, None)
                columns.finish()
                meanwhile()
                second([0])
                next_rows.finish(second)
                if core == 0:
                    sent(columns, rows, next_rows)

        comm.next_recv = comm.most_recv

    def largest(over):
        kept = edge[0]
        sends = []
        for axis, at in (("y", 1), ("x", 1 + ny), ("c", 1 + ny + nx)):
            edge[at] = kept
            index, send = over if axis == "c" else comm.recv_index(), comm.send_index()
            for d in range(1, n[axis]):
                comm.start(edge.at[at], edge.at[at + d], axis, around(me[axis], d, n[axis]), index, send)
            yield
            comm.wait(edge.at[pl.ds(at + 1, n[axis] - 1)], index, axis, around(me[axis], 1, n[axis]))
            comm.wait_sent(edge.at[pl.ds(at + 1, n[axis] - 1)], send, axis, around(me[axis], 1, n[axis]))
            for d in range(1, n[axis]):
                kept = jnp.maximum(kept, edge[at + d])
        peaks[...] = kept

    def put(value, rp, cp):
        value = value.astype(BF)
        if rp is not None:
            rp[z] = value
        if cp is not None:
            cp[y, c, x] = value

    def times(rps, cp, core=None, totals=None):
        def step(k, totals):
            at = k if core is None else k * nc + core
            right = cp[at // nc, at % nc].reshape(nx * ph, pw)
            return tuple(t + jnp.dot(rp[at], right, preferred_element_type=F32) for t, rp in zip(totals, rps))

        if totals is None:
            totals = tuple(jnp.zeros((ph, pw), F32) for _ in rps)
        return lax.fori_loop(0, nz if core is None else nz // nc, step, totals)

    def with_identity(value, row, column, scale):
        rows = lax.broadcasted_iota(jnp.int32, value.shape, 0) + row
        across = lax.broadcasted_iota(jnp.int32, value.shape, 1) + column
        return value + jnp.where(rows == across, scale, 0.0)

    put(gram[...], rpg, cpg)

    def first_half():
        (sums[...],) = times([rpg], cpg, c)

    gather_panels(rpg, cpg, first_half)

    def sizes(k, total):
        return total + jnp.abs(rpg[k].astype(F32))

    row_sums = jnp.sum(lax.fori_loop(0, nz, sizes, jnp.zeros((ph, pw), F32)), axis=1, keepdims=True)
    edge[0] = jnp.broadcast_to(jnp.max(row_sums, axis=0, keepdims=True), edge.shape[1:])
    (square,) = times([rpg], cpg, 1 - c, (sums[...],))
    sums[...] = square
    put(square, rp2, cp2)

    def scales():
        bound = jnp.max(jnp.max(peaks[...], axis=1, keepdims=True), axis=0, keepdims=True) + epsilon
        return 1.0 / bound, lax.rsqrt(bound)

    def mix(once, twice, inverse, row, column):
        value = second_coef * (once.astype(F32) * inverse) + third_coef * (twice.astype(F32) * inverse * inverse)
        return with_identity(value, row, column, first_coef)

    def mixed_columns():
        inverse, _ = scales()

        def step(k, carry):
            at = (k // (nc * nx), k // nx % nc, k % nx)
            cpp[at] = mix(cpg[at], cp2[at], inverse, k * ph, z * pw).astype(BF)
            return carry

        lax.fori_loop(0, ny * nc * nx, step, 0)
        cube[...] = mix(gram[...], sums[...], inverse, mine * ph, z * pw)

    def rows_of_product(k):
        inverse, _ = scales()
        once = rpg[k].astype(F32) * inverse
        twice = rp2[k].astype(F32) * inverse * inverse
        thrice = rp3[k].astype(F32) * inverse * inverse * inverse
        return (first_coef * once + second_coef * twice + third_coef * thrice).astype(BF)

    two_products(
        rp2, cp2, adding(lambda k: rp2[k], cpg), rp3, lambda value: value, mixed_columns, adding(rows_of_product, cpp), peak=True
    )
    put(total_ref[...], rpn, cpn)

    def next_first(value):
        sums[...] = value
        return value

    two_products(
        rpn, cpn, adding(lambda k: rpn[k], cpp), rpw, next_first, lambda: None, adding(lambda k: rpw[k], cpn)
    )
    _, root = scales()
    whole = (gain * root) * (first_coef * cube[...] + second_coef * sums[...] + third_coef * total_ref[...])
    qi[z, x] = whole.astype(BF)

    def share_of(d):
        k = around(z, d, nz)
        left = qi[k].reshape(rows_half, pw)
        for side in range(nc):
            product[side] += jnp.dot(left, right_rows(around(c, 1 - side, nc), k), preferred_element_type=F32)

    product[...] = jnp.zeros(product.shape, F32)
    base_recv, base_send = comm.next_recv, comm.next_send

    def q(d, e, h=None):
        ref = qi.at[around(z, d, nz), around(x, e, nx)]
        return two_halves(ref, h, half_rows)

    def to_z(d, e, way, index, send, h=None):
        comm.start(q(d, e, h), q(d, e, h), "z", around(z, way, nz), index, send)

    def to_x(d, e, way, index, send, h=None):
        comm.start(q(d, e, h), q(d, e, h), "x", around(x, way, nx), index, send)

    def gather_z_first():
        z_send, x_send = comm.send_index(), comm.send_index()
        far, near, three, four = {w: comm.recv_index() for w in (1, -1)}, comm.recv_index(), comm.recv_index(), comm.recv_index()
        groups = {0: [0], 1: [-1, 1], 2: [-2, 2], 3: [-3, 3], 4: [4]}
        hop = {(g, w): comm.recv_index() for g in groups for w in (1, -1)}
        last = {g: comm.recv_index() for g in groups}

        def spread(g, ds):
            for d in ds:
                for w in (1, -1):
                    to_x(d, 0, w, hop[g, w], x_send)
                if g == 4:
                    to_x(d, 0, 2, last[g], x_send)

        def pass_on(g):
            for w in (1, -1):
                take(len(groups[g]), hop[g, w], "x")
                if g < 4:
                    for d in groups[g]:
                        to_x(d, -w, w, last[g], x_send, 0 if w > 0 else 1)

        def finish(g):
            take(len(groups[g]), last[g], "x")
            for d in groups[g]:
                share_of(d)

        for w in (1, -1):
            to_z(0, 0, 2 * w, far[w], z_send)
        for w in (1, -1):
            to_z(0, 0, w, near, z_send)
        spread(0, [0])
        for w in (1, -1):
            take(1, far[w], "z")
            to_z(-2 * w, 0, w, three, z_send)
            to_z(-2 * w, 0, 2 * w, four, z_send, 0 if w > 0 else 1)
            spread(2, [-2 * w])
        take(2, near, "z")
        spread(1, groups[1])
        pass_on(0)
        take(2, three, "z")
        spread(3, groups[3])
        take(1, four, "z")
        spread(4, [4])
        pass_on(2)
        pass_on(1)
        finish(0)
        pass_on(3)
        finish(2)
        finish(1)
        pass_on(4)
        finish(3)
        finish(4)
        take_sent(7, z_send, "z")
        take_sent(24, x_send, "x")

    def gather_x_first():
        x_send, z_send = comm.send_index(), comm.send_index()
        near_x, far_x = comm.recv_index(), comm.recv_index()
        groups = {0: [0], 1: [-1, 1]}
        chain = {(g, h, w): comm.recv_index() for g in groups for h in range(1, 4) for w in (1, -1)}
        chain.update({(g, 4, w): k for g in groups for k in [comm.recv_index()] for w in (1, -1)})
        far, near, three, four = {w: comm.recv_index() for w in (1, -1)}, comm.recv_index(), comm.recv_index(), comm.recv_index()

        def go(g, h):
            for w in (1, -1):
                if h > 1:
                    take(len(groups[g]), chain[g, h - 1, w], "z")
                for e in groups[g]:
                    to_z(-w * (h - 1), e, w, chain[g, h, w], z_send, None if h < 4 else 0 if w > 0 else 1)

        to_x(0, 0, 2, far_x, x_send)
        for w in (1, -1):
            to_x(0, 0, w, near_x, x_send)
        go(0, 1)
        take(2, near_x, "x")
        go(1, 1)
        take(1, far_x, "x")
        for w in (1, -1):
            to_z(0, 2, 2 * w, far[w], z_send)
        for w in (1, -1):
            to_z(0, 2, w, near, z_send)
        go(0, 2)
        share_of(0)
        go(1, 2)
        go(0, 3)
        for w in (1, -1):
            take(1, far[w], "z")
            to_z(-2 * w, 2, w, three, z_send)
            to_z(-2 * w, 2, 2 * w, four, z_send, 0 if w > 0 else 1)
        go(1, 3)
        take(2, near, "z")
        share_of(-1)
        share_of(1)
        go(0, 4)
        share_of(-2)
        share_of(2)
        go(1, 4)
        take(2, three, "z")
        share_of(-3)
        share_of(3)
        take(1, four, "z")
        take(1, chain[0, 4, 1], "z")
        take(2, chain[1, 4, 1], "z")
        share_of(4)
        take_sent(3, x_send, "x")
        take_sent(28, z_send, "z")

    def take_sent(count, send, axis):
        comm.wait_sent(blocks(count), send, axis, around(me[axis], 1, n[axis]))

    for core in range(nc):

        @pl.when(c == core)
        def _():
            comm.next_recv, comm.next_send = base_recv, base_send
            (gather_z_first if core == 0 else gather_x_first)()

    comm.next_recv = comm.most_recv
    swap[0] = product[0].astype(BF)
    index = comm.start(swap.at[0], swap.at[1], "c", 1 - c)
    o_ref[pl.ds(top, rows_half)] = product[1].astype(BF)
    comm.wait(swap.at[1], index, "c", 1 - c)
    o_ref[pl.ds(pl.multiple_of((1 - c) * rows_half, rows_half), rows_half)] = swap[1]
    comm.drain()
    for count, send, axis in unsent:
        comm.wait_sent(rpg.at[pl.ds(0, count)] if count < nz else blocks(count), send, axis, around(me[axis], 1, n[axis]))


def update_call(n, gain, x):
    nz, nx, nc, ny = n["z"], n["x"], n["c"], n["y"]
    rows_block, columns = x.shape
    rows = rows_block * ny
    ph, pw = rows // (ny * nc * nx), rows // nz
    row_panel = pltpu.VMEM((nz, ph, pw), BF)
    column_panel = pltpu.VMEM((ny, nc, nx, ph, pw), BF)
    hops_z, hops_x = max(nz // 2, 1), max(nx // 2, 1)
    tiles = 2 + ny + nx + nc
    return pl.pallas_call(
        lambda *refs: kernel(n, gain, *refs),
        out_shape=jax.ShapeDtypeStruct(x.shape, BF),
        in_specs=[pl.BlockSpec(memory_space=pltpu.VMEM)],
        out_specs=pl.BlockSpec(memory_space=pltpu.VMEM),
        scratch_shapes=[
            pltpu.VMEM((nc, ny, rows_block, columns), BF),
            pltpu.VMEM((nz, nx, ph, pw), BF),
            pltpu.VMEM((2, hops_z, nx, ph, pw), BF),
            pltpu.VMEM((2, hops_x, nz, ph, pw), BF),
            pltpu.VMEM((nz - 1, ph, pw), BF),
            pltpu.VMEM((nx - 1, ph, pw), BF),
            pltpu.VMEM((ph, pw), F32),
            pltpu.VMEM((ph, pw), F32),
            pltpu.VMEM((ph, pw), F32),
            pltpu.VMEM((ph, pw), F32),
            row_panel, column_panel, row_panel, column_panel, row_panel, column_panel,
            row_panel, column_panel, row_panel,
            pltpu.VMEM((nz, nx, ph, pw), BF),
            pltpu.VMEM((nc, rows_block // nc, columns), F32),
            pltpu.VMEM((2, rows_block // nc, columns), BF),
            pltpu.VMEM((tiles, 8, 128), F32),
            pltpu.VMEM((8, 128), F32),
            pltpu.SemaphoreType.DMA((80,)),
            pltpu.SemaphoreType.DMA((300,)),
            pltpu.SemaphoreType.DMA,
        ],
        compiler_params=pltpu.CompilerParams(
            collective_id=0, has_side_effects=True, vmem_limit_bytes=48 * 1024 * 1024
        ),
    )(x)


def per_device(grad, momentum):
    new_momentum = momentum_beta * momentum + grad.astype(F32)
    iterate = (grad.astype(F32) + momentum_beta * new_momentum).astype(BF)
    update = update_call(SIZES, shape_gain * math.sqrt(max(R, C)), iterate)
    return (update, new_momentum)


def solution(mesh):
    devices = mesh.devices.reshape(SIZES["z"], SIZES["x"], SIZES["c"], SIZES["y"])
    split = Mesh(devices, (AX["z"], AX["x"], AX["c"], AX["y"]))
    mats = (AX["z"], AX["x"], AX["c"])
    return jax.shard_map(
        per_device,
        mesh=split,
        in_specs=(P(AX["y"], mats), P(AX["y"], mats)),
        out_specs=(P(AX["y"], mats), P(AX["y"], mats)),
        check_vma=False,
    )
```

```python
import math

import jax
import jax.numpy as jnp
from jax import lax
from jax.experimental import pallas as pl
from jax.experimental.pallas import tpu as pltpu
from jax.sharding import Mesh
from jax.sharding import PartitionSpec as P

R = 3072
C = 16384
AX = {"z": "mats_0", "x": "mats_1", "c": "mats_2", "y": "tp"}
SIZES = {"z": 8, "x": 4, "c": 2, "y": 4}

momentum_beta = 0.95
first_coef = 3.4445
second_coef = -4.775
third_coef = 2.0315
shape_gain = 0.2
epsilon = 1e-06

BF = jnp.bfloat16
F32 = jnp.float32
MESH = pl.DeviceIdType.MESH


def around(s, d, n):
    d = d % n
    return s if d == 0 else lax.rem(s + d, n)


class Comm:
    def __init__(self, send_sems, recv_sems):
        self.send_sems, self.recv_sems = send_sems, recv_sems
        self.next_send = self.next_recv = self.most_recv = 0
        self.open = []

    def recv_index(self):
        self.next_recv += 1
        self.most_recv = max(self.most_recv, self.next_recv)
        return self.next_recv - 1

    def send_index(self):
        self.next_send += 1
        return self.next_send - 1

    def start(self, src, dst, axis, to, index=None, send=None):
        if index is None:
            index = self.recv_index()
        kept = send is None
        if kept:
            send = self.send_index()
        copy = pltpu.make_async_remote_copy(
            src_ref=src,
            dst_ref=dst,
            send_sem=self.send_sems.at[send],
            recv_sem=self.recv_sems.at[index],
            device_id={AX[axis]: to},
            device_id_type=MESH,
        )
        copy.start()
        if kept:
            self.open.append(copy)
        return index

    def handle(self, ref, send, index, axis, peer):
        return pltpu.make_async_remote_copy(
            src_ref=ref,
            dst_ref=ref,
            send_sem=self.send_sems.at[send],
            recv_sem=self.recv_sems.at[index],
            device_id={AX[axis]: peer},
            device_id_type=MESH,
        )

    def wait(self, ref, index, axis, peer):
        self.handle(ref, 0, index, axis, peer).wait_recv()

    def wait_sent(self, ref, send, axis, peer):
        self.handle(ref, send, 0, axis, peer).wait_send()

    def drain(self):
        for copy in self.open:
            copy.wait_send()
        self.next_send -= len(self.open)
        self.open = []


def kernel(
    n, gain, x_ref, o_ref, xc, part, z1, x1, z2, x2, gram, cube, sums, total_ref, rpg, cpg, rp2, cp2, rp3, cpp, rpn, cpn, rpw,
    qi, product, swap, edge, peaks, send_sems, recv_sems, local_sem,
):
    nz, nx, nc, ny = n["z"], n["x"], n["c"], n["y"]
    me = {a: (lax.axis_index(AX[a]) if n[a] > 1 else 0) for a in "zxcy"}
    z, x, c, y = me["z"], me["x"], me["c"], me["y"]
    rows_block, columns = x_ref.shape
    rows_half = rows_block // nc
    ph, pw = gram.shape
    half_rows = ph // 2
    mine = (y * nc + c) * nx + x
    comm = Comm(send_sems, recv_sems)

    barrier = pltpu.get_barrier_semaphore()
    peers = [(a, d) for a in "zxcy" for d in range(1, n[a]) if a != "z" or d in (1, 2, nz - 2, nz - 1)]
    for a, d in peers:
        pl.semaphore_signal(barrier, inc=1, device_id={AX[a]: around(me[a], d, n[a])}, device_id_type=MESH)
    pl.semaphore_wait(barrier, len(peers))

    own = pltpu.make_async_copy(x_ref, xc.at[c, y], local_sem)
    own.start()
    quarter = rows_block // 4
    x_send, x_over_send, x_over = comm.send_index(), comm.send_index(), comm.recv_index()
    came = {(w, k): comm.recv_index() for w in (1, -1) for k in range(5)}

    def block(d, k, count=1):
        return xc.at[c, around(y, d, ny), pl.ds(k * quarter, count * quarter)]

    def to_y(ref, dst, w, k):
        comm.start(ref, dst, "y", around(y, w, ny), came[w, k], x_send)

    def from_y(w, k, ref):
        comm.wait(ref, came[w, k], "y", around(y, -w, ny))

    def to_other(d, k, count):
        comm.start(block(d, k, count), block(d, k, count), "c", 1 - c, x_over, x_over_send)

    for k in range(4):
        for w, q in ((1, k), (-1, 3 - k)):
            to_y(x_ref.at[pl.ds(q * quarter, quarter)], block(0, q), w, min(k, 2))
    comm.start(x_ref, xc.at[c, y], "c", 1 - c, x_over, x_over_send)
    for k in range(2):
        for w, q in ((1, k), (-1, 3 - k)):
            from_y(w, k, block(-w, q))
            to_y(block(-w, q), block(-w, q), w, 3 + k)
    to_other(-1, 0, 2)
    to_other(1, 2, 2)
    from_y(1, 2, block(-1, 2, 2))
    to_other(-1, 2, 2)
    from_y(-1, 2, block(1, 0, 2))
    to_other(1, 0, 2)
    for k in range(2):
        for w, q in ((1, k), (-1, 3 - k)):
            from_y(w, 3 + k, block(2, q))
            to_other(2, q, 1)
    own.wait()
    comm.wait(xc.at[1 - c], x_over, "c", 1 - c)
    comm.wait_sent(xc.at[c, pl.ds(0, 3)], x_send, "y", around(y, 1, ny))
    comm.wait_sent(xc.at[c], x_over_send, "c", 1 - c)

    per_block = rows_block // pw
    top = pl.multiple_of(c * rows_half, rows_half)

    def right_rows(h, d):
        return xc[h, d // per_block, pl.ds(pl.multiple_of(d % per_block * pw, pw), pw)]

    def outer(left, right):
        return lax.dot_general(left, right, (((1,), (1,)), ((), ())), preferred_element_type=F32)

    def part_columns(d):
        total = sum(outer(xc[h, y, pl.ds(top, rows_half)], right_rows(h, d)) for h in range(nc))
        part[d] = total.astype(BF).reshape(nx, ph, pw)

    def part_rows(d):
        rows = pl.ds(pl.multiple_of(top + d * ph, ph), ph)

        def step(k, carry):
            part[k, d] = sum(outer(xc[h, y, rows], right_rows(h, k)) for h in range(nc)).astype(BF)
            return carry

        lax.fori_loop(0, nz, step, 0)

    def plus(piece, *more):
        total = piece[...].astype(F32)
        for other in more:
            total += other[...].astype(F32)
        return total

    def plane_sum(axis, piece, landing, chunks, prepare, finish):
        size, s = n[axis], me[axis]
        last = size // 2
        halves = {1: chunks[: len(chunks) // 2], -1: chunks[len(chunks) // 2 :]}
        index = {}
        send = comm.send_index()

        def go(way, hop, e):
            index[way, hop, e] = comm.recv_index()
            d = around(s, way * (last - hop + 1), size)
            comm.start(piece(d, e), landing(way, hop, e), axis, around(s, way, size), index[way, hop, e], send)

        def come(way, hop, e):
            comm.wait(landing(way, hop, e), index[way, hop, e], axis, around(s, -way, size))
            return landing(way, hop, e)

        prepare(around(s, last, size))
        for a, b in zip(halves[1], halves[-1]):
            go(1, 1, a)
            go(-1, 1, b)
        for hop in range(2, last + 1):
            for way in (1, -1):
                prepare(around(s, way * (last - hop + 1), size))
                if hop == 2:
                    for e in halves[-way]:
                        go(way, hop, e)
            for k in range(len(chunks)):
                for way in (1, -1):
                    order = halves[way] if hop == 2 else halves[-way] + halves[way]
                    if k < len(order):
                        e = order[k]
                        ref = piece(around(s, way * (last - hop + 1), size), e)
                        ref[...] = plus(ref, come(way, hop - 1, e)).astype(BF)
                        go(way, hop, e)
        prepare(s)

        def summed(e):
            return plus(piece(s, e), come(1, last, e), come(-1, last, e))

        finish(summed, lambda e: piece(s, e))
        comm.wait_sent(blocks((size - 1) * len(chunks)), send, axis, around(s, 1, size))

    def straight_to_x(summed, kept):
        index, send = comm.recv_index(), comm.send_index()
        for e in (2, 3, 1, 0):
            if e == 0:
                gram[...] = summed(e)
            else:
                kept(e)[...] = summed(e).astype(BF)
                comm.start(kept(e), x2.at[e - 1], "x", around(x, e, nx), index, send)
        comm.wait(x2, index, "x", around(x, 1, nx))
        gram[...] = plus(gram, *(x2.at[k] for k in range(nx - 1)))
        comm.wait_sent(x2, send, "x", around(x, 1, nx))

    def two_hops_to_z(summed, kept):
        send, end = comm.send_index(), comm.recv_index()
        three = {w: comm.recv_index() for w in (1, -1)}
        four = {w: comm.recv_index() for w in (1, -1)}

        def go(ref, slot, index, way):
            comm.start(ref, slot, "z", around(z, way, nz), index, send)

        for e in (4, 3, 5, 6, 2, 1, 7):
            kept(e)[...] = summed(e).astype(BF)
            if e == 4:
                for w in (1, -1):
                    h = 0 if w > 0 else 1
                    go(two_halves(kept(4), h, half_rows), two_halves(z2.at[2], h, half_rows), four[w], 2 * w)
            elif e in (3, 5):
                w = 1 if e == 3 else -1
                go(kept(e), z2.at[0 if w > 0 else 1], three[w], w)
            elif e in (1, 7):
                w = 1 if e == 1 else -1
                go(kept(e), z2.at[3 if w > 0 else 4], end, w)
        gram[...] = summed(0)
        for w in (1, -1):
            mid = kept(2 * w % nz)
            slot, h = z2.at[0 if w > 0 else 1], 0 if w > 0 else 1
            comm.wait(slot, three[w], "z", around(z, -w, nz))
            mid[...] = plus(mid, slot).astype(BF)
            half = two_halves(z2.at[2], h, half_rows)
            comm.wait(half, four[w], "z", around(z, -2 * w, nz))
            part_of = two_halves(mid, h, half_rows)
            part_of[...] = plus(part_of, half).astype(BF)
            go(mid, z2.at[5 if w > 0 else 6], end, 2 * w)
        comm.wait(z2.at[pl.ds(3, 4)], end, "z", around(z, 1, nz))
        gram[...] = plus(gram, *(z2.at[k] for k in range(3, 7)))
        comm.wait_sent(z2, send, "z", around(z, 1, nz))

    def two_halves(ref, h, length):
        return ref if h is None else ref.at[pl.ds(h * length, length)]

    def blocks(count):
        across = next(k for k in range(nx, 0, -1) if count % k == 0 and count // k <= nz)
        return part.at[pl.ds(0, count // across), pl.ds(0, across)]

    base_recv, base_send = comm.next_recv, comm.next_send
    for core in range(nc):

        @pl.when(c == core)
        def _():
            comm.next_recv, comm.next_send = base_recv, base_send
            if core == 0:
                plane_sum(
                    "z", lambda d, e: part.at[d, around(x, e, nx)], lambda way, hop, e: z1.at[int(way > 0), hop - 1, e],
                    [2, 1, 3, 0], part_columns, straight_to_x,
                )
            else:
                plane_sum(
                    "x", lambda d, e: part.at[around(z, e, nz), d], lambda way, hop, e: x1.at[int(way > 0), hop - 1, e],
                    [4, 5, 2, 7, 3, 6, 1, 0], part_rows, two_hops_to_z,
                )

    comm.next_recv = comm.most_recv

    unsent = []

    def take(count, index, axis):
        comm.wait(blocks(count), index, axis, around(me[axis], 1, n[axis]))

    class Rows:
        def __init__(self, rp):
            self.rp, self.send = rp, comm.send_index()
            self.near, self.rest, self.far = comm.recv_index(), comm.recv_index(), {w: comm.recv_index() for w in (1, -1)}

        def to(self, d, way, index, h=None):
            ref = two_halves(self.rp.at[around(z, d, nz)], h, half_rows)
            comm.start(ref, ref, "z", around(z, way, nz), index, self.send)

        def begin(self):
            for w in (1, -1):
                self.to(0, 2 * w, self.far[w])
            for w in (1, -1):
                self.to(0, w, self.near)

        def forward(self):
            for w in (1, -1):
                take(1, self.far[w], "z")
                self.to(-2 * w, 2 * w, self.rest, 0 if w > 0 else 1)
                self.to(-2 * w, w, self.rest)

        def finish(self, use=lambda ds: None):
            use([-2, 2])
            take(2, self.near, "z")
            use([-1, 1])
            take(3, self.rest, "z")
            use([-3, 3, 4])

    class Columns:
        def __init__(self, core, cp):
            self.core, self.cp = core, cp
            self.a1, self.a2 = ("y", "x") if core == 0 else ("x", "y")
            self.over, self.send_over, self.send = comm.recv_index(), comm.send_index(), comm.send_index()
            self.near, self.far, self.last = comm.recv_index(), comm.recv_index(), comm.recv_index()
            self.hop = {(w, k): comm.recv_index() for w in (1, -1) for k in range(3)}

        def at1(self, d):
            return around(me[self.a1], d, n[self.a1])

        def at2(self, d):
            return around(me[self.a2], d, n[self.a2])

        def spot(self, d1, d2, h=None):
            iy, ix = (self.at1(d1), self.at2(d2)) if self.a1 == "y" else (self.at2(d2), self.at1(d1))
            return two_halves(self.cp.at[iy, self.core, ix], h, half_rows)

        def to_partner(self, d2):
            ref = self.cp.at[:, self.core, self.at2(d2)] if self.a1 == "y" else self.cp.at[self.at2(d2), self.core]
            comm.start(ref, ref, "c", 1 - c, self.over, self.send_over)

        def spread(self, d1, k):
            ref = self.spot(d1, 0)
            for w in (1, -1):
                comm.start(ref, ref, self.a2, self.at2(w), self.hop[w, k], self.send)
            if d1 == 2:
                comm.start(ref, ref, self.a2, self.at2(2), self.last, self.send)

        def pass_on(self, w, d1s):
            for d1 in d1s:
                half = self.spot(d1, -w, 0 if w > 0 else 1)
                comm.start(half, half, self.a2, self.at2(w), self.last, self.send)

        def begin(self):
            own = self.spot(0, 0)
            comm.start(own, own, self.a1, self.at1(2), self.far, self.send)
            for w in (1, -1):
                comm.start(own, own, self.a1, self.at1(w), self.near, self.send)

        def first(self):
            take(2, self.near, self.a1)
            self.spread(-1, 1)
            self.spread(1, 1)
            for w in (1, -1):
                take(1, self.hop[w, 0], self.a2)
                self.pass_on(w, [0])
            take(1, self.far, self.a1)
            self.spread(2, 2)
            self.to_partner(0)

        def middle(self):
            for w in (1, -1):
                take(2, self.hop[w, 1], self.a2)
                self.pass_on(w, [-1, 1])
            for w in (1, -1):
                take(1, self.hop[w, 2], self.a2)
                self.to_partner(-w)

        def end(self):
            take(4, self.last, self.a2)
            self.to_partner(2)

        def finish(self):
            take(16, self.over, "c")

    def gather_panels(rp, cp, half_done):
        base_recv, base_send = comm.next_recv, comm.next_send
        for core in range(nc):

            @pl.when(c == core)
            def _():
                comm.next_recv, comm.next_send = base_recv, base_send
                columns, rows = Columns(core, cp), Rows(rp)
                columns.begin()
                rows.begin()
                columns.spread(0, 0)
                columns.first()
                rows.forward()
                columns.middle()
                rows.finish()
                columns.end()
                half_done()
                columns.finish()
                if core == 0:
                    sent(columns, rows)

        comm.next_recv = comm.most_recv

    def sent(columns, *rows):
        unsent.append((15, columns.send, "y"))
        unsent.append((16, columns.send_over, "c"))
        unsent.extend((7, each.send, "z") for each in rows)

    def adding(left, cp):
        def use(ds):
            total = total_ref[...]
            for d in ds:
                k = around(z, d, nz)
                total += jnp.dot(left(k), cp[k // nc, k % nc].reshape(nx * ph, pw), preferred_element_type=F32)
            total_ref[...] = total

        return use

    def two_products(rp, cp, first, rp_next, next_piece, meanwhile, second, peak=False):
        base_recv, base_send = comm.next_recv, comm.next_send
        for core in range(nc):

            @pl.when(c == core)
            def _():
                comm.next_recv, comm.next_send = base_recv, base_send
                columns, rows = Columns(core, cp), Rows(rp)
                peak_walk = largest(comm.recv_index()) if peak else iter(())
                rows.begin()
                columns.begin()
                columns.spread(0, 0)
                next(peak_walk, None)
                total_ref[...] = jnp.zeros(total_ref.shape, F32)
                first([0])
                rows.forward()
                columns.first()
                next(peak_walk, None)
                rows.finish(first)
                rp_next[z] = next_piece(total_ref[...]).astype(BF)
                next_rows = Rows(rp_next)
                next_rows.begin()
                total_ref[...] = jnp.zeros(total_ref.shape, F32)
                columns.middle()
                next(peak_walk, None)
                next_rows.forward()
                columns.end()
                next(peak_walk, None)
                columns.finish()
                meanwhile()
                second([0])
                next_rows.finish(second)
                if core == 0:
                    sent(columns, rows, next_rows)

        comm.next_recv = comm.most_recv

    def largest(over):
        kept = edge[0]
        sends = []
        for axis, at in (("y", 1), ("x", 1 + ny), ("c", 1 + ny + nx)):
            edge[at] = kept
            index, send = over if axis == "c" else comm.recv_index(), comm.send_index()
            for d in range(1, n[axis]):
                comm.start(edge.at[at], edge.at[at + d], axis, around(me[axis], d, n[axis]), index, send)
            yield
            comm.wait(edge.at[pl.ds(at + 1, n[axis] - 1)], index, axis, around(me[axis], 1, n[axis]))
            comm.wait_sent(edge.at[pl.ds(at + 1, n[axis] - 1)], send, axis, around(me[axis], 1, n[axis]))
            for d in range(1, n[axis]):
                kept = jnp.maximum(kept, edge[at + d])
        peaks[...] = kept

    def put(value, rp, cp):
        value = value.astype(BF)
        if rp is not None:
            rp[z] = value
        if cp is not None:
            cp[y, c, x] = value

    def times(rps, cp, core=None, totals=None):
        def step(k, totals):
            at = k if core is None else k * nc + core
            right = cp[at // nc, at % nc].reshape(nx * ph, pw)
            return tuple(t + jnp.dot(rp[at], right, preferred_element_type=F32) for t, rp in zip(totals, rps))

        if totals is None:
            totals = tuple(jnp.zeros((ph, pw), F32) for _ in rps)
        return lax.fori_loop(0, nz if core is None else nz // nc, step, totals)

    def with_identity(value, row, column, scale):
        rows = lax.broadcasted_iota(jnp.int32, value.shape, 0) + row
        across = lax.broadcasted_iota(jnp.int32, value.shape, 1) + column
        return value + jnp.where(rows == across, scale, 0.0)

    put(gram[...], rpg, cpg)

    def sizes(k, total):
        return total + jnp.abs(rpg[k].astype(F32))

    def first_half():
        (sums[...],) = times([rpg], cpg, c)
        row_sums = jnp.sum(lax.fori_loop(0, nz, sizes, jnp.zeros((ph, pw), F32)), axis=1, keepdims=True)
        edge[0] = jnp.broadcast_to(jnp.max(row_sums, axis=0, keepdims=True), edge.shape[1:])
        product[...] = jnp.zeros(product.shape, F32)

    gather_panels(rpg, cpg, first_half)
    (square,) = times([rpg], cpg, 1 - c, (sums[...],))
    sums[...] = square
    put(square, rp2, cp2)

    def scales():
        bound = jnp.max(jnp.max(peaks[...], axis=1, keepdims=True), axis=0, keepdims=True) + epsilon
        return 1.0 / bound, lax.rsqrt(bound)

    def mix(once, twice, inverse, row, column):
        value = second_coef * (once.astype(F32) * inverse) + third_coef * (twice.astype(F32) * inverse * inverse)
        return with_identity(value, row, column, first_coef)

    def mixed_columns():
        inverse, _ = scales()

        def step(k, carry):
            at = (k // (nc * nx), k // nx % nc, k % nx)
            cpp[at] = mix(cpg[at], cp2[at], inverse, k * ph, z * pw).astype(BF)
            return carry

        lax.fori_loop(0, ny * nc * nx, step, 0)
        cube[...] = mix(gram[...], sums[...], inverse, mine * ph, z * pw)

    def rows_of_product(k):
        inverse, _ = scales()
        once = rpg[k].astype(F32) * inverse
        twice = rp2[k].astype(F32) * inverse * inverse
        thrice = rp3[k].astype(F32) * inverse * inverse * inverse
        return (first_coef * once + second_coef * twice + third_coef * thrice).astype(BF)

    two_products(
        rp2, cp2, adding(lambda k: rp2[k], cpg), rp3, lambda value: value, mixed_columns, adding(rows_of_product, cpp), peak=True
    )
    put(total_ref[...], rpn, cpn)

    def next_first(value):
        sums[...] = value
        return value

    two_products(
        rpn, cpn, adding(lambda k: rpn[k], cpp), rpw, next_first, lambda: None, adding(lambda k: rpw[k], cpn)
    )
    _, root = scales()
    whole = (gain * root) * (first_coef * cube[...] + second_coef * sums[...] + third_coef * total_ref[...])
    qi[z, x] = whole.astype(BF)

    def share_of(d):
        k = around(z, d, nz)
        left = qi[k].reshape(rows_half, pw)
        for side in range(nc):
            product[side] += jnp.dot(left, right_rows(around(c, 1 - side, nc), k), preferred_element_type=F32)

    base_recv, base_send = comm.next_recv, comm.next_send

    def q(d, e, h=None):
        ref = qi.at[around(z, d, nz), around(x, e, nx)]
        return two_halves(ref, h, half_rows)

    def to_z(d, e, way, index, send, h=None):
        comm.start(q(d, e, h), q(d, e, h), "z", around(z, way, nz), index, send)

    def to_x(d, e, way, index, send, h=None):
        comm.start(q(d, e, h), q(d, e, h), "x", around(x, way, nx), index, send)

    def gather_z_first():
        z_send, x_send = comm.send_index(), comm.send_index()
        far, near, three, four = {w: comm.recv_index() for w in (1, -1)}, comm.recv_index(), comm.recv_index(), comm.recv_index()
        groups = {0: [0], 1: [-1, 1], 2: [-2, 2], 3: [-3, 3], 4: [4]}
        hop = {(g, w): comm.recv_index() for g in groups for w in (1, -1)}
        last = {g: comm.recv_index() for g in groups}

        def spread(g, ds):
            for d in ds:
                for w in (1, -1):
                    to_x(d, 0, w, hop[g, w], x_send)
                if g == 4:
                    to_x(d, 0, 2, last[g], x_send)

        def pass_on(g):
            for w in (1, -1):
                take(len(groups[g]), hop[g, w], "x")
                if g < 4:
                    for d in groups[g]:
                        to_x(d, -w, w, last[g], x_send, 0 if w > 0 else 1)

        def finish(g):
            take(len(groups[g]), last[g], "x")
            for d in groups[g]:
                share_of(d)

        for w in (1, -1):
            to_z(0, 0, 2 * w, far[w], z_send)
        for w in (1, -1):
            to_z(0, 0, w, near, z_send)
        spread(0, [0])
        for w in (1, -1):
            take(1, far[w], "z")
            to_z(-2 * w, 0, w, three, z_send)
            to_z(-2 * w, 0, 2 * w, four, z_send, 0 if w > 0 else 1)
            spread(2, [-2 * w])
        take(2, near, "z")
        spread(1, groups[1])
        pass_on(0)
        take(2, three, "z")
        spread(3, groups[3])
        take(1, four, "z")
        spread(4, [4])
        pass_on(2)
        pass_on(1)
        finish(0)
        pass_on(3)
        finish(2)
        finish(1)
        pass_on(4)
        finish(3)
        finish(4)
        take_sent(7, z_send, "z")
        take_sent(24, x_send, "x")

    def gather_x_first():
        x_send, z_send = comm.send_index(), comm.send_index()
        near_x, far_x = comm.recv_index(), comm.recv_index()
        groups = {0: [0], 1: [-1, 1]}
        chain = {(g, h, w): comm.recv_index() for g in groups for h in range(1, 4) for w in (1, -1)}
        chain.update({(g, 4, w): k for g in groups for k in [comm.recv_index()] for w in (1, -1)})
        far, near, three, four = {w: comm.recv_index() for w in (1, -1)}, comm.recv_index(), comm.recv_index(), comm.recv_index()

        def go(g, h):
            for w in (1, -1):
                if h > 1:
                    take(len(groups[g]), chain[g, h - 1, w], "z")
                for e in groups[g]:
                    to_z(-w * (h - 1), e, w, chain[g, h, w], z_send, None if h < 4 else 0 if w > 0 else 1)

        to_x(0, 0, 2, far_x, x_send)
        for w in (1, -1):
            to_x(0, 0, w, near_x, x_send)
        go(0, 1)
        take(2, near_x, "x")
        go(1, 1)
        take(1, far_x, "x")
        for w in (1, -1):
            to_z(0, 2, 2 * w, far[w], z_send)
        for w in (1, -1):
            to_z(0, 2, w, near, z_send)
        go(0, 2)
        share_of(0)
        go(1, 2)
        go(0, 3)
        for w in (1, -1):
            take(1, far[w], "z")
            to_z(-2 * w, 2, w, three, z_send)
            to_z(-2 * w, 2, 2 * w, four, z_send, 0 if w > 0 else 1)
        go(1, 3)
        take(2, near, "z")
        share_of(-1)
        share_of(1)
        go(0, 4)
        share_of(-2)
        share_of(2)
        go(1, 4)
        take(2, three, "z")
        share_of(-3)
        share_of(3)
        take(1, four, "z")
        take(1, chain[0, 4, 1], "z")
        take(2, chain[1, 4, 1], "z")
        share_of(4)
        take_sent(3, x_send, "x")
        take_sent(28, z_send, "z")

    def take_sent(count, send, axis):
        comm.wait_sent(blocks(count), send, axis, around(me[axis], 1, n[axis]))

    for core in range(nc):

        @pl.when(c == core)
        def _():
            comm.next_recv, comm.next_send = base_recv, base_send
            (gather_z_first if core == 0 else gather_x_first)()

    comm.next_recv = comm.most_recv
    swap[0] = product[0].astype(BF)
    index = comm.start(swap.at[0], swap.at[1], "c", 1 - c)
    o_ref[pl.ds(top, rows_half)] = product[1].astype(BF)
    comm.wait(swap.at[1], index, "c", 1 - c)
    o_ref[pl.ds(pl.multiple_of((1 - c) * rows_half, rows_half), rows_half)] = swap[1]
    comm.drain()
    for count, send, axis in unsent:
        comm.wait_sent(rpg.at[pl.ds(0, count)] if count < nz else blocks(count), send, axis, around(me[axis], 1, n[axis]))


def update_call(n, gain, x):
    nz, nx, nc, ny = n["z"], n["x"], n["c"], n["y"]
    rows_block, columns = x.shape
    rows = rows_block * ny
    ph, pw = rows // (ny * nc * nx), rows // nz
    row_panel = pltpu.VMEM((nz, ph, pw), BF)
    column_panel = pltpu.VMEM((ny, nc, nx, ph, pw), BF)
    hops_z, hops_x = max(nz // 2, 1), max(nx // 2, 1)
    tiles = 2 + ny + nx + nc
    return pl.pallas_call(
        lambda *refs: kernel(n, gain, *refs),
        out_shape=jax.ShapeDtypeStruct(x.shape, BF),
        in_specs=[pl.BlockSpec(memory_space=pltpu.VMEM)],
        out_specs=pl.BlockSpec(memory_space=pltpu.VMEM),
        scratch_shapes=[
            pltpu.VMEM((nc, ny, rows_block, columns), BF),
            pltpu.VMEM((nz, nx, ph, pw), BF),
            pltpu.VMEM((2, hops_z, nx, ph, pw), BF),
            pltpu.VMEM((2, hops_x, nz, ph, pw), BF),
            pltpu.VMEM((nz - 1, ph, pw), BF),
            pltpu.VMEM((nx - 1, ph, pw), BF),
            pltpu.VMEM((ph, pw), F32),
            pltpu.VMEM((ph, pw), F32),
            pltpu.VMEM((ph, pw), F32),
            pltpu.VMEM((ph, pw), F32),
            row_panel, column_panel, row_panel, column_panel, row_panel, column_panel,
            row_panel, column_panel, row_panel,
            pltpu.VMEM((nz, nx, ph, pw), BF),
            pltpu.VMEM((nc, rows_block // nc, columns), F32),
            pltpu.VMEM((2, rows_block // nc, columns), BF),
            pltpu.VMEM((tiles, 8, 128), F32),
            pltpu.VMEM((8, 128), F32),
            pltpu.SemaphoreType.DMA((80,)),
            pltpu.SemaphoreType.DMA((300,)),
            pltpu.SemaphoreType.DMA,
        ],
        compiler_params=pltpu.CompilerParams(
            collective_id=0, has_side_effects=True, vmem_limit_bytes=48 * 1024 * 1024
        ),
    )(x)


def per_device(grad, momentum):
    new_momentum = momentum_beta * momentum + grad.astype(F32)
    iterate = (grad.astype(F32) + momentum_beta * new_momentum).astype(BF)
    update = update_call(SIZES, shape_gain * math.sqrt(max(R, C)), iterate)
    return (update, new_momentum)


def solution(mesh):
    devices = mesh.devices.reshape(SIZES["z"], SIZES["x"], SIZES["c"], SIZES["y"])
    split = Mesh(devices, (AX["z"], AX["x"], AX["c"], AX["y"]))
    mats = (AX["z"], AX["x"], AX["c"])
    return jax.shard_map(
        per_device,
        mesh=split,
        in_specs=(P(AX["y"], mats), P(AX["y"], mats)),
        out_specs=(P(AX["y"], mats), P(AX["y"], mats)),
        check_vma=False,
    )
```
